8 devices in a mesh: row: 2 (over z, y), col: 4 (over x, core).
Axes of the slice: x: 2, y: 2, z: 1, core: 2. Of those that a mesh axis runs over, the one named last changes fastest.
Arguments:
- w_one: float32 [2, 4, 4, 384, 1536], P('row', 'col')
- w_two: float32 [2, 4, 4, 1536, 384], P('row', 'col')
- inputs: bfloat16 [2, 4, 3, 2048, 384], P('row', 'col')
- targets: bfloat16 [2, 4, 3, 2048, 384], P('row', 'col')
Outputs:
- output 1: float32 [2, 4, 4, 384, 1536], P('row', 'col')
- output 2: float32 [2, 4, 4, 1536, 384], P('row', 'col')
All inputs are finite; a program needn't handle non-finite values.
Results may differ from the reference program's by a relative error of at most 0.00188.
Values are sent between devices in bfloat16 or wider.
A program may use at most 1 GiB of HBM per device.

```python
import jax
import jax.numpy as jnp
from jax import lax

GRID_ROWS = 2
GRID_COLS = 4
LAYERS = 4
NUM_STEPS = 3
BATCH_ROWS = 2048
D_MODEL = 384
D_FF = 1536

LEARN_RATE = 1.5
NORM_EPS = 1e-6
GELU_C = 0.7978845608028654
GELU_K = 0.044715
REPLICA_SPREAD = 0.5


def gelu_value(pre_act):
    tanh_inner = jnp.tanh(GELU_C * (pre_act + GELU_K * pre_act * pre_act * pre_act))
    return 0.5 * pre_act * (1.0 + tanh_inner)


def gelu_slope(pre_act):
    tanh_inner = jnp.tanh(GELU_C * (pre_act + GELU_K * pre_act * pre_act * pre_act))
    return 0.5 * (1.0 + tanh_inner) + 0.5 * pre_act * (1.0 - tanh_inner * tanh_inner) * GELU_C * (1.0 + 3.0 * GELU_K * pre_act * pre_act)


def setup_inputs(seed: int = 0) -> dict:
    root_key = jax.random.key(seed)
    sub_keys = jax.random.split(root_key, 6)
    grid_shape = (GRID_ROWS, GRID_COLS)
    shape_one = (LAYERS, D_MODEL, D_FF)
    shape_two = (LAYERS, D_FF, D_MODEL)
    norm_fac = (1.0 + REPLICA_SPREAD * REPLICA_SPREAD) ** -0.5
    base_one = jax.random.normal(sub_keys[0], shape_one, jnp.float32)
    own_one = jax.random.normal(sub_keys[1], grid_shape + shape_one, jnp.float32)
    w_one = (base_one + REPLICA_SPREAD * own_one) * (norm_fac * D_MODEL ** -0.5)
    base_two = jax.random.normal(sub_keys[2], shape_two, jnp.float32)
    own_two = jax.random.normal(sub_keys[3], grid_shape + shape_two, jnp.float32)
    w_two = (base_two + REPLICA_SPREAD * own_two) * (norm_fac * D_FF ** -0.5)
    data_shape = grid_shape + (NUM_STEPS, BATCH_ROWS, D_MODEL)
    inputs = jax.random.normal(sub_keys[4], data_shape, jnp.float32).astype(jnp.bfloat16)
    targets = jax.random.normal(sub_keys[5], data_shape, jnp.float32).astype(jnp.bfloat16)
    return {'w_one': w_one, 'w_two': w_two, 'inputs': inputs, 'targets': targets}


def local_update(w_one, w_two, x_in, target):
    one_lo = w_one.astype(jnp.bfloat16)
    two_lo = w_two.astype(jnp.bfloat16)
    hidden = x_in
    saved_acts = []
    for layer_idx in range(LAYERS):
        hid_f = hidden.astype(jnp.float32)
        inv_rms = lax.rsqrt(jnp.mean(hid_f * hid_f, axis=-1, keepdims=True) + NORM_EPS)
        normed = hid_f * inv_rms
        normed_lo = normed.astype(jnp.bfloat16)
        pre_act = jnp.dot(normed_lo, one_lo[layer_idx], preferred_element_type=jnp.float32)
        act_lo = gelu_value(pre_act).astype(jnp.bfloat16)
        mlp_out = jnp.dot(act_lo, two_lo[layer_idx], preferred_element_type=jnp.float32)
        saved_acts.append((normed, inv_rms, normed_lo, pre_act, act_lo))
        hidden = (hid_f + mlp_out).astype(jnp.bfloat16)
    d_hidden = (2.0 / (BATCH_ROWS * D_MODEL)) * (hidden.astype(jnp.float32) - target.astype(jnp.float32))
    grads_one = [None] * LAYERS
    grads_two = [None] * LAYERS
    for layer_idx in reversed(range(LAYERS)):
        normed, inv_rms, normed_lo, pre_act, act_lo = saved_acts[layer_idx]
        d_lo = d_hidden.astype(jnp.bfloat16)
        grads_two[layer_idx] = jnp.dot(act_lo.T, d_lo, preferred_element_type=jnp.float32)
        d_act = jnp.dot(d_lo, two_lo[layer_idx].T, preferred_element_type=jnp.float32)
        d_pre = (d_act * gelu_slope(pre_act)).astype(jnp.bfloat16)
        grads_one[layer_idx] = jnp.dot(normed_lo.T, d_pre, preferred_element_type=jnp.float32)
        if layer_idx > 0:
            d_normed = jnp.dot(d_pre, one_lo[layer_idx].T, preferred_element_type=jnp.float32)
            d_hidden = d_hidden + inv_rms * (d_normed - normed * jnp.mean(d_normed * normed, axis=-1, keepdims=True))
    return w_one - LEARN_RATE * jnp.stack(grads_one), w_two - LEARN_RATE * jnp.stack(grads_two)


def gossip_mix(upd_vals):
    wire_vals = upd_vals.astype(jnp.bfloat16)
    mix_sum = upd_vals + jnp.roll(wire_vals, 1, axis=1).astype(jnp.float32)
    mix_sum = mix_sum + jnp.roll(wire_vals, -1, axis=1).astype(jnp.float32)
    mix_sum = mix_sum + jnp.roll(wire_vals, 1, axis=0).astype(jnp.float32)
    mix_sum = mix_sum + jnp.roll(wire_vals, -1, axis=0).astype(jnp.float32)
    return mix_sum / 5.0


def reference(w_one, w_two, inputs, targets):
    n_rep = GRID_ROWS * GRID_COLS
    for step_idx in range(NUM_STEPS):
        flat_one = w_one.reshape((n_rep, LAYERS, D_MODEL, D_FF))
        flat_two = w_two.reshape((n_rep, LAYERS, D_FF, D_MODEL))
        x_step = inputs[:, :, step_idx].reshape((n_rep, BATCH_ROWS, D_MODEL))
        t_step = targets[:, :, step_idx].reshape((n_rep, BATCH_ROWS, D_MODEL))
        upd_one, upd_two = lax.map(lambda packed: local_update(packed[0], packed[1], packed[2], packed[3]), (flat_one, flat_two, x_step, t_step))
        w_one = gossip_mix(upd_one.reshape(w_one.shape))
        w_two = gossip_mix(upd_two.reshape(w_two.shape))
    return w_one, w_two
```

```python
import functools

import jax
import jax.numpy as jnp
from jax import lax
from jax.experimental import pallas as pl
from jax.experimental.pallas import tpu as pltpu
from jax.sharding import PartitionSpec as P

LEARN_RATE = 1.5
NORM_EPS = 1e-6
GELU_C = 0.7978845608028654
GELU_K = 0.044715

MESH = pl.DeviceIdType.MESH
F32 = jnp.float32
BF16 = jnp.bfloat16
CHUNKS = 3
TILE = 512


def matmul(lhs, rhs):
    return jnp.dot(lhs, rhs, preferred_element_type=F32)


def matmul_t(lhs, rhs):
    return lax.dot_general(lhs, rhs, (((1,), (1,)), ((), ())), preferred_element_type=F32)


def gelu_half(pre_act):
    sq = pre_act * pre_act
    t = jnp.tanh(pre_act * (GELU_C + (GELU_C * GELU_K) * sq))
    return sq, t, 0.5 + 0.5 * t


def inv_rms_of(hid_f):
    return lax.rsqrt(jnp.mean(hid_f * hid_f, axis=-1, keepdims=True) + NORM_EPS)


def kernel(dims, w1_hbm, w2_hbm, x_hbm, tgt_hbm, o1_hbm, o2_hbm, r1_hbm, r2_hbm,
           m1, m2, l1, l2, hs, err, acc, tgt, act, dpre, nrm, err_lo, nrm_t, err_t, st1, st2,
           load_sem, data_sem, stage_sem, out_sem, send_sem, recv_sem):
    n_rows, n_cols, n_steps, n_layers, batch, d_model, d_ff = dims
    f_blk = d_ff // CHUNKS
    n_blk = n_layers * CHUNKS
    n_tiles = batch // TILE
    row, col = lax.axis_index("row"), lax.axis_index("col")
    peers = ((row, lax.rem(col + 1, n_cols)), (row, lax.rem(col + n_cols - 1, n_cols)), (n_rows - 1 - row, col))

    def cols_of(blk):
        return pl.ds(pl.multiple_of(lax.rem(blk, CHUNKS) * f_blk, f_blk), f_blk)

    def load_copies(blk):
        layer = lax.div(blk, CHUNKS)
        return (pltpu.make_async_copy(w1_hbm.at[layer, :, cols_of(blk)], m1.at[blk], load_sem.at[blk, 0]),
                pltpu.make_async_copy(w2_hbm.at[layer, cols_of(blk), :], m2.at[blk], load_sem.at[blk, 1]))

    def out_copies(blk):
        layer = lax.div(blk, CHUNKS)
        return (pltpu.make_async_copy(m1.at[blk], o1_hbm.at[layer, :, cols_of(blk)], out_sem.at[blk, 0]),
                pltpu.make_async_copy(m2.at[blk], o2_hbm.at[layer, cols_of(blk), :], out_sem.at[blk, 1]))

    def data_copies(step):
        return (pltpu.make_async_copy(x_hbm.at[step], hs.at[0], data_sem.at[0]),
                pltpu.make_async_copy(tgt_hbm.at[step], tgt, data_sem.at[1]))

    def sends(step, blk):
        out = []
        for slot, peer in enumerate(peers):
            for mat, (src, dst) in enumerate(((l2, r2_hbm), (l1, r1_hbm))):
                out.append(pltpu.make_async_remote_copy(
                    src_ref=src.at[blk], dst_ref=dst.at[step, slot, blk],
                    send_sem=send_sem.at[blk, mat, slot], recv_sem=recv_sem.at[step, blk, mat, slot],
                    device_id=peer, device_id_type=MESH))
        return out

    def start_sends(step, blk):
        for cp in sends(step, blk):
            cp.start()

    def sent_early(blk):
        layer, chunk = lax.div(blk, CHUNKS), lax.rem(blk, CHUNKS)
        head = jnp.logical_and(chunk == 0, layer > 0)
        return jnp.logical_or(head, blk == n_blk - 2)

    def tile_rows(i):
        return pl.ds(pl.multiple_of(i * TILE, TILE), TILE)

    def mix(step, blk):
        for cp in sends(step, blk):
            cp.wait_recv()
        stage = []
        for slot in range(3):
            stage.append(pltpu.make_async_copy(r1_hbm.at[step, slot, blk], st1.at[slot], stage_sem.at[0, slot]))
            stage.append(pltpu.make_async_copy(r2_hbm.at[step, slot, blk], st2.at[slot], stage_sem.at[1, slot]))
        for cp in stage:
            cp.start()
        for cp in sends(step, blk):
            cp.wait_send()
        for cp in stage:
            cp.wait()
        for own, lo, st in ((m1, l1, st1), (m2, l2, st2)):
            other = st[2].astype(F32)
            new = (own[blk] + st[0].astype(F32) + st[1].astype(F32) + other + other) * 0.2
            own[blk] = new
            lo[blk] = new.astype(BF16)

    barrier = pltpu.get_barrier_semaphore()
    for peer in peers:
        pl.semaphore_signal(barrier, inc=1, device_id=peer, device_id_type=MESH)
    for cp in data_copies(0):
        cp.start()

    @pl.loop(0, n_blk)
    def _(blk):
        for cp in load_copies(blk):
            cp.start()

    pl.semaphore_wait(barrier, 3)

    @pl.loop(0, n_steps)
    def _(step):
        for cp in data_copies(step):
            cp.wait()

        @pl.loop(0, n_blk)
        def _(blk):
            layer, chunk = lax.div(blk, CHUNKS), lax.rem(blk, CHUNKS)

            @pl.when(chunk == 0)
            def _():
                @pl.loop(0, n_tiles)
                def _(i):
                    rows = tile_rows(i)
                    hid_f = hs[layer, rows, :].astype(F32)
                    nrm[rows, :] = (hid_f * inv_rms_of(hid_f)).astype(BF16)
                    acc[rows, :] = hid_f

            @pl.when(step == 0)
            def _():
                for cp in load_copies(blk):
                    cp.wait()
                l1[blk] = m1[blk].astype(BF16)
                l2[blk] = m2[blk].astype(BF16)

            @pl.when(step > 0)
            def _():
                mix(step - 1, blk)

            @pl.loop(0, n_tiles)
            def _(i):
                rows = tile_rows(i)
                pre = matmul(nrm[rows, :], l1[blk])
                _, _, half = gelu_half(pre)
                acc[rows, :] += matmul((pre * half).astype(BF16), l2[blk])

            @pl.when(jnp.logical_and(chunk == CHUNKS - 1, layer < n_layers - 1))
            def _():
                @pl.loop(0, n_tiles)
                def _(i):
                    rows = tile_rows(i)
                    hs[lax.min(layer + 1, n_layers - 1), rows, :] = acc[rows, :].astype(BF16)

        @pl.loop(0, n_tiles)
        def _(i):
            rows = tile_rows(i)
            hid = acc[rows, :].astype(BF16).astype(F32)
            err[rows, :] = (2.0 / (batch * d_model)) * (hid - tgt[rows, :].astype(F32))

        @pl.loop(0, n_blk)
        def _(k):
            layer, chunk = n_layers - 1 - lax.div(k, CHUNKS), lax.rem(k, CHUNKS)
            blk = layer * CHUNKS + chunk

            @pl.when(chunk == 0)
            def _():
                @pl.loop(0, n_tiles)
                def _(i):
                    rows = tile_rows(i)
                    hid_f = hs[layer, rows, :].astype(F32)
                    n_f = hid_f * inv_rms_of(hid_f)
                    nrm[rows, :] = n_f.astype(BF16)
                    nrm_t[:, rows] = n_f.T.astype(BF16)
                    e_f = err[rows, :]
                    err_lo[rows, :] = e_f.astype(BF16)
                    err_t[:, rows] = e_f.T.astype(BF16)
                    acc[rows, :] = jnp.zeros((TILE, d_model), F32)

            @pl.loop(0, n_tiles)
            def _(i):
                rows = tile_rows(i)
                pre = matmul(nrm[rows, :], l1[blk])
                sq, t, half = gelu_half(pre)
                act[rows, :] = (pre * half).astype(BF16)
                slope = half + ((half * (1.0 - t)) * pre) * (GELU_C + (3.0 * GELU_C * GELU_K) * sq)
                d_pre = (matmul_t(err_lo[rows, :], l2[blk]) * slope).astype(BF16)
                dpre[rows, :] = d_pre
                acc[rows, :] += matmul_t(d_pre, l1[blk])

            grad_two = matmul(err_t[...], act[...]).T
            upd_two = m2[blk] - LEARN_RATE * grad_two
            m2[blk] = upd_two
            l2[blk] = upd_two.astype(BF16)
            grad_one = matmul(nrm_t[...], dpre[...])
            upd_one = m1[blk] - LEARN_RATE * grad_one
            m1[blk] = upd_one
            l1[blk] = upd_one.astype(BF16)

            @pl.when(sent_early(blk))
            def _():
                start_sends(step, blk)

            @pl.when(jnp.logical_and(chunk == CHUNKS - 1, layer > 0))
            def _():
                @pl.loop(0, n_tiles)
                def _(i):
                    rows = tile_rows(i)
                    hid_f = hs[layer, rows, :].astype(F32)
                    inv = inv_rms_of(hid_f)
                    n_f = hid_f * inv
                    d_n = acc[rows, :]
                    err[rows, :] += inv * (d_n - n_f * jnp.mean(d_n * n_f, axis=-1, keepdims=True))

        @pl.loop(0, n_blk)
        def _(blk):
            @pl.when(jnp.logical_not(sent_early(blk)))
            def _():
                start_sends(step, blk)

        @pl.when(step < n_steps - 1)
        def _():
            for cp in data_copies(lax.min(step + 1, n_steps - 1)):
                cp.start()

    for early in (True, False):
        @pl.loop(0, n_blk)
        def _(blk):
            turn = sent_early(blk) if early else jnp.logical_not(sent_early(blk))

            @pl.when(turn)
            def _():
                mix(n_steps - 1, blk)
                for cp in out_copies(blk):
                    cp.start()

    @pl.loop(0, n_blk)
    def _(blk):
        for cp in out_copies(blk):
            cp.wait()


def solution(mesh):
    n_rows = mesh.shape['row']
    n_cols = mesh.shape['col']

    def device_fn(w_one, w_two, inputs, targets):
        n_layers, d_model, d_ff = w_one.shape[2:]
        n_steps, batch = inputs.shape[2:4]
        f_blk = d_ff // CHUNKS
        n_blk = n_layers * CHUNKS
        dims = (n_rows, n_cols, n_steps, n_layers, batch, d_model, d_ff)
        any_spec = pl.BlockSpec(memory_space=pl.ANY)
        out = pl.pallas_call(
            functools.partial(kernel, dims),
            out_shape=(
                jax.ShapeDtypeStruct((n_layers, d_model, d_ff), F32),
                jax.ShapeDtypeStruct((n_layers, d_ff, d_model), F32),
                jax.ShapeDtypeStruct((n_steps, 3, n_blk, d_model, f_blk), BF16),
                jax.ShapeDtypeStruct((n_steps, 3, n_blk, f_blk, d_model), BF16),
            ),
            in_specs=[any_spec] * 4,
            out_specs=(any_spec,) * 4,
            scratch_shapes=[
                pltpu.VMEM((n_blk, d_model, f_blk), F32),
                pltpu.VMEM((n_blk, f_blk, d_model), F32),
                pltpu.VMEM((n_blk, d_model, f_blk), BF16),
                pltpu.VMEM((n_blk, f_blk, d_model), BF16),
                pltpu.VMEM((n_layers, batch, d_model), BF16),
                pltpu.VMEM((batch, d_model), F32),
                pltpu.VMEM((batch, d_model), F32),
                pltpu.VMEM((batch, d_model), BF16),
                pltpu.VMEM((batch, f_blk), BF16),
                pltpu.VMEM((batch, f_blk), BF16),
                pltpu.VMEM((batch, d_model), BF16),
                pltpu.VMEM((batch, d_model), BF16),
                pltpu.VMEM((d_model, batch), BF16),
                pltpu.VMEM((d_model, batch), BF16),
                pltpu.VMEM((3, d_model, f_blk), BF16),
                pltpu.VMEM((3, f_blk, d_model), BF16),
                pltpu.SemaphoreType.DMA((n_blk, 2)),
                pltpu.SemaphoreType.DMA((2,)),
                pltpu.SemaphoreType.DMA((2, 3)),
                pltpu.SemaphoreType.DMA((n_blk, 2)),
                pltpu.SemaphoreType.DMA((n_blk, 2, 3)),
                pltpu.SemaphoreType.DMA((n_steps, n_blk, 2, 3)),
            ],
            compiler_params=pltpu.CompilerParams(
                collective_id=0, has_side_effects=True, vmem_limit_bytes=67_043_328),
            name="gossip_sgd",
        )(w_one[0, 0], w_two[0, 0], inputs[0, 0], targets[0, 0])
        return out[0][None, None], out[1][None, None]

    grid_spec = P('row', 'col')
    return jax.shard_map(device_fn, mesh=mesh, in_specs=(grid_spec,) * 4, out_specs=(grid_spec, grid_spec), check_vma=False)
```

```python
import functools

import jax
import jax.numpy as jnp
from jax import lax
from jax.experimental import pallas as pl
from jax.experimental.pallas import tpu as pltpu
from jax.sharding import PartitionSpec as P

LEARN_RATE = 1.5
NORM_EPS = 1e-6
GELU_C = 0.7978845608028654
GELU_K = 0.044715

MESH = pl.DeviceIdType.MESH
F32 = jnp.float32
BF16 = jnp.bfloat16
CHUNKS = 3
TILE = 512


def matmul(lhs, rhs):
    return jnp.dot(lhs, rhs, preferred_element_type=F32)


def matmul_t(lhs, rhs):
    return lax.dot_general(lhs, rhs, (((1,), (1,)), ((), ())), preferred_element_type=F32)


def gelu_half(pre_act):
    sq = pre_act * pre_act
    t = jnp.tanh(pre_act * (GELU_C + (GELU_C * GELU_K) * sq))
    return sq, t, 0.5 + 0.5 * t


def inv_rms_of(hid_f):
    return lax.rsqrt(jnp.mean(hid_f * hid_f, axis=-1, keepdims=True) + NORM_EPS)


def kernel(dims, w1_hbm, w2_hbm, x_hbm, tgt_hbm, o1_hbm, o2_hbm, r1_hbm, r2_hbm,
           m1, m2, l1, l2, hs, err, acc, tgt, act, dpre, nrm, err_lo, nrm_t, err_t, head_two, st1, st2,
           load_sem, data_sem, stage_sem, out_sem, send_sem, recv_sem):
    n_rows, n_cols, n_steps, n_layers, batch, d_model, d_ff = dims
    f_blk = d_ff // CHUNKS
    n_blk = n_layers * CHUNKS
    n_tiles = batch // TILE
    row, col = lax.axis_index("row"), lax.axis_index("col")
    peers = ((row, lax.rem(col + 1, n_cols)), (row, lax.rem(col + n_cols - 1, n_cols)), (n_rows - 1 - row, col))

    def cols_of(blk):
        return pl.ds(pl.multiple_of(lax.rem(blk, CHUNKS) * f_blk, f_blk), f_blk)

    def load_copies(blk):
        layer = lax.div(blk, CHUNKS)
        return (pltpu.make_async_copy(w1_hbm.at[layer, :, cols_of(blk)], m1.at[blk], load_sem.at[blk, 0]),
                pltpu.make_async_copy(w2_hbm.at[layer, cols_of(blk), :], m2.at[blk], load_sem.at[blk, 1]))

    def out_copies(blk):
        layer = lax.div(blk, CHUNKS)
        return (pltpu.make_async_copy(m1.at[blk], o1_hbm.at[layer, :, cols_of(blk)], out_sem.at[blk, 0]),
                pltpu.make_async_copy(m2.at[blk], o2_hbm.at[layer, cols_of(blk), :], out_sem.at[blk, 1]))

    def data_copies(step):
        return (pltpu.make_async_copy(x_hbm.at[step], hs.at[0], data_sem.at[0]),
                pltpu.make_async_copy(tgt_hbm.at[step], tgt, data_sem.at[1]))

    wires = ((m1, l1, r1_hbm, st1), (m2, l2, r2_hbm, st2))

    def sends(step, blk, mat, src=None):
        out = []
        for slot, peer in enumerate(peers):
            out.append(pltpu.make_async_remote_copy(
                src_ref=wires[mat][1].at[blk] if src is None else src, dst_ref=wires[mat][2].at[step, slot, blk],
                send_sem=send_sem.at[blk, mat, slot], recv_sem=recv_sem.at[step, blk, mat, slot],
                device_id=peer, device_id_type=MESH))
        return out

    def start_sends(step, blk, mat, src=None):
        for cp in sends(step, blk, mat, src):
            cp.start()

    def sent_early(blk):
        layer, chunk = lax.div(blk, CHUNKS), lax.rem(blk, CHUNKS)
        return jnp.logical_and(chunk < CHUNKS - 1, layer > 0)

    def tile_rows(i):
        return pl.ds(pl.multiple_of(i * TILE, TILE), TILE)

    def mix(step, blk, mats=(0, 1)):
        for mat in mats:
            for cp in sends(step, blk, mat):
                cp.wait_recv()
        stage = [pltpu.make_async_copy(wires[mat][2].at[step, slot, blk], wires[mat][3].at[slot], stage_sem.at[mat, slot])
                 for mat in mats for slot in range(3)]
        for cp in stage:
            cp.start()
        for mat in mats:
            for cp in sends(step, blk, mat):
                cp.wait_send()
        for cp in stage:
            cp.wait()
        for mat in mats:
            own, lo, _, st = wires[mat]
            other = st[2].astype(F32)
            new = (own[blk] + st[0].astype(F32) + st[1].astype(F32) + other + other) * 0.2
            own[blk] = new
            lo[blk] = new.astype(BF16)

    barrier = pltpu.get_barrier_semaphore()
    for peer in peers:
        pl.semaphore_signal(barrier, inc=1, device_id=peer, device_id_type=MESH)
    for cp in data_copies(0):
        cp.start()

    @pl.loop(0, n_blk)
    def _(blk):
        for cp in load_copies(blk):
            cp.start()

    pl.semaphore_wait(barrier, 3)

    @pl.loop(0, n_steps)
    def _(step):
        for cp in data_copies(step):
            cp.wait()

        @pl.when(step > 0)
        def _():
            @pl.loop(0, n_blk)
            def _(k):
                blk = n_blk - CHUNKS - CHUNKS * lax.div(k, CHUNKS) + lax.rem(k, CHUNKS)

                @pl.when(sent_early(blk))
                def _():
                    mix(step - 1, blk)

        @pl.loop(0, n_blk)
        def _(blk):
            layer, chunk = lax.div(blk, CHUNKS), lax.rem(blk, CHUNKS)

            @pl.when(chunk == 0)
            def _():
                @pl.loop(0, n_tiles)
                def _(i):
                    rows = tile_rows(i)
                    hid_f = hs[layer, rows, :].astype(F32)
                    n_f = hid_f * inv_rms_of(hid_f)
                    nrm[rows, :] = n_f.astype(BF16)
                    acc[rows, :] = hid_f

                    @pl.when(layer == n_layers - 1)
                    def _():
                        nrm_t[:, rows] = n_f.T.astype(BF16)

            @pl.when(step == 0)
            def _():
                for cp in load_copies(blk):
                    cp.wait()
                l1[blk] = m1[blk].astype(BF16)
                l2[blk] = m2[blk].astype(BF16)

            last_blk = blk == n_blk - 1
            halves = jnp.logical_and(step > 0, last_blk)

            @pl.when(jnp.logical_and(step > 0, jnp.logical_not(jnp.logical_or(sent_early(blk), last_blk))))
            def _():
                mix(step - 1, blk)

            @pl.when(jnp.logical_not(halves))
            def _():
                @pl.loop(0, n_tiles)
                def _(i):
                    rows = tile_rows(i)
                    pre = matmul(nrm[rows, :], l1[blk])
                    _, _, half = gelu_half(pre)
                    a_lo = (pre * half).astype(BF16)
                    acc[rows, :] += matmul(a_lo, l2[blk])

                    @pl.when(blk == n_blk - CHUNKS)
                    def _():
                        act[rows, :] = a_lo

            @pl.when(halves)
            def _():
                mix(step - 1, blk, (0,))

                @pl.loop(0, n_tiles)
                def _(i):
                    rows = tile_rows(i)
                    pre = matmul(nrm[rows, :], l1[blk])
                    _, _, half = gelu_half(pre)
                    dpre[rows, :] = (pre * half).astype(BF16)

                mix(step - 1, blk, (1,))

                @pl.loop(0, n_tiles)
                def _(i):
                    rows = tile_rows(i)
                    acc[rows, :] += matmul(dpre[rows, :], l2[blk])

            @pl.when(jnp.logical_and(chunk == CHUNKS - 1, layer < n_layers - 1))
            def _():
                @pl.loop(0, n_tiles)
                def _(i):
                    rows = tile_rows(i)
                    hs[lax.min(layer + 1, n_layers - 1), rows, :] = acc[rows, :].astype(BF16)

        @pl.loop(0, n_tiles)
        def _(i):
            rows = tile_rows(i)
            hid = acc[rows, :].astype(BF16).astype(F32)
            e_f = (2.0 / (batch * d_model)) * (hid - tgt[rows, :].astype(F32))
            err[rows, :] = e_f
            err_lo[rows, :] = e_f.astype(BF16)
            err_t[:, rows] = e_f.T.astype(BF16)
            acc[rows, :] = jnp.zeros((TILE, d_model), F32)

        head_blk = n_blk - CHUNKS
        upd_head = m2[head_blk] - LEARN_RATE * matmul(err_t[...], act[...]).T
        m2[head_blk] = upd_head
        head_two[...] = upd_head.astype(BF16)
        start_sends(step, head_blk, 1, head_two)

        @pl.loop(0, n_blk)
        def _(k):
            layer, chunk = n_layers - 1 - lax.div(k, CHUNKS), lax.rem(k, CHUNKS)
            blk = layer * CHUNKS + chunk

            @pl.when(jnp.logical_and(chunk == 0, k > 0))
            def _():
                @pl.loop(0, n_tiles)
                def _(i):
                    rows = tile_rows(i)
                    hid_f = hs[layer, rows, :].astype(F32)
                    n_f = hid_f * inv_rms_of(hid_f)
                    nrm[rows, :] = n_f.astype(BF16)
                    nrm_t[:, rows] = n_f.T.astype(BF16)
                    e_f = err[rows, :]
                    err_lo[rows, :] = e_f.astype(BF16)
                    err_t[:, rows] = e_f.T.astype(BF16)
                    acc[rows, :] = jnp.zeros((TILE, d_model), F32)

            @pl.loop(0, n_tiles)
            def _(i):
                rows = tile_rows(i)
                pre = matmul(nrm[rows, :], l1[blk])
                sq, t, half = gelu_half(pre)
                act[rows, :] = (pre * half).astype(BF16)
                slope = half + ((half * (1.0 - t)) * pre) * (GELU_C + (3.0 * GELU_C * GELU_K) * sq)
                d_pre = (matmul_t(err_lo[rows, :], l2[blk]) * slope).astype(BF16)
                dpre[rows, :] = d_pre
                acc[rows, :] += matmul_t(d_pre, l1[blk])

            @pl.when(k > 0)
            def _():
                upd_two = m2[blk] - LEARN_RATE * matmul(err_t[...], act[...]).T
                m2[blk] = upd_two
                l2[blk] = upd_two.astype(BF16)

                @pl.when(sent_early(blk))
                def _():
                    start_sends(step, blk, 1)

            grad_one = matmul(nrm_t[...], dpre[...])
            upd_one = m1[blk] - LEARN_RATE * grad_one
            m1[blk] = upd_one
            l1[blk] = upd_one.astype(BF16)

            @pl.when(sent_early(blk))
            def _():
                start_sends(step, blk, 0)

            @pl.when(jnp.logical_and(chunk == CHUNKS - 1, layer > 0))
            def _():
                @pl.loop(0, n_tiles)
                def _(i):
                    rows = tile_rows(i)
                    hid_f = hs[layer, rows, :].astype(F32)
                    inv = inv_rms_of(hid_f)
                    n_f = hid_f * inv
                    d_n = acc[rows, :]
                    err[rows, :] += inv * (d_n - n_f * jnp.mean(d_n * n_f, axis=-1, keepdims=True))

        @pl.loop(0, n_blk)
        def _(blk):
            @pl.when(jnp.logical_not(sent_early(blk)))
            def _():
                start_sends(step, blk, 0)
                start_sends(step, blk, 1)

        @pl.when(step < n_steps - 1)
        def _():
            for cp in data_copies(lax.min(step + 1, n_steps - 1)):
                cp.start()

    for early in (True, False):
        @pl.loop(0, n_blk)
        def _(blk):
            turn = sent_early(blk) if early else jnp.logical_not(sent_early(blk))

            @pl.when(turn)
            def _():
                mix(n_steps - 1, blk)
                for cp in out_copies(blk):
                    cp.start()

    @pl.loop(0, n_blk)
    def _(blk):
        for cp in out_copies(blk):
            cp.wait()


def solution(mesh):
    n_rows = mesh.shape['row']
    n_cols = mesh.shape['col']

    def device_fn(w_one, w_two, inputs, targets):
        n_layers, d_model, d_ff = w_one.shape[2:]
        n_steps, batch = inputs.shape[2:4]
        f_blk = d_ff // CHUNKS
        n_blk = n_layers * CHUNKS
        dims = (n_rows, n_cols, n_steps, n_layers, batch, d_model, d_ff)
        any_spec = pl.BlockSpec(memory_space=pl.ANY)
        out = pl.pallas_call(
            functools.partial(kernel, dims),
            out_shape=(
                jax.ShapeDtypeStruct((n_layers, d_model, d_ff), F32),
                jax.ShapeDtypeStruct((n_layers, d_ff, d_model), F32),
                jax.ShapeDtypeStruct((n_steps, 3, n_blk, d_model, f_blk), BF16),
                jax.ShapeDtypeStruct((n_steps, 3, n_blk, f_blk, d_model), BF16),
            ),
            in_specs=[any_spec] * 4,
            out_specs=(any_spec,) * 4,
            scratch_shapes=[
                pltpu.VMEM((n_blk, d_model, f_blk), F32),
                pltpu.VMEM((n_blk, f_blk, d_model), F32),
                pltpu.VMEM((n_blk, d_model, f_blk), BF16),
                pltpu.VMEM((n_blk, f_blk, d_model), BF16),
                pltpu.VMEM((n_layers, batch, d_model), BF16),
                pltpu.VMEM((batch, d_model), F32),
                pltpu.VMEM((batch, d_model), F32),
                pltpu.VMEM((batch, d_model), BF16),
                pltpu.VMEM((batch, f_blk), BF16),
                pltpu.VMEM((batch, f_blk), BF16),
                pltpu.VMEM((batch, d_model), BF16),
                pltpu.VMEM((batch, d_model), BF16),
                pltpu.VMEM((d_model, batch), BF16),
                pltpu.VMEM((d_model, batch), BF16),
                pltpu.VMEM((f_blk, d_model), BF16),
                pltpu.VMEM((3, d_model, f_blk), BF16),
                pltpu.VMEM((3, f_blk, d_model), BF16),
                pltpu.SemaphoreType.DMA((n_blk, 2)),
                pltpu.SemaphoreType.DMA((2,)),
                pltpu.SemaphoreType.DMA((2, 3)),
                pltpu.SemaphoreType.DMA((n_blk, 2)),
                pltpu.SemaphoreType.DMA((n_blk, 2, 3)),
                pltpu.SemaphoreType.DMA((n_steps, n_blk, 2, 3)),
            ],
            compiler_params=pltpu.CompilerParams(
                collective_id=0, has_side_effects=True, vmem_limit_bytes=67_043_328),
            name="gossip_sgd",
        )(w_one[0, 0], w_two[0, 0], inputs[0, 0], targets[0, 0])
        return out[0][None, None], out[1][None, None]

    grid_spec = P('row', 'col')
    return jax.shard_map(device_fn, mesh=mesh, in_specs=(grid_spec,) * 4, out_specs=(grid_spec, grid_spec), check_vma=False)
```

```python
import functools

import jax
import jax.numpy as jnp
from jax import lax
from jax.experimental import pallas as pl
from jax.experimental.pallas import tpu as pltpu
from jax.sharding import PartitionSpec as P

LEARN_RATE = 1.5
NORM_EPS = 1e-6
GELU_C = 0.7978845608028654
GELU_K = 0.044715

MESH = pl.DeviceIdType.MESH
F32 = jnp.float32
BF16 = jnp.bfloat16
CHUNKS = 3
TILE = 512
SUB = 256


def matmul(lhs, rhs):
    return jnp.dot(lhs, rhs, preferred_element_type=F32)


def matmul_t(lhs, rhs):
    return lax.dot_general(lhs, rhs, (((1,), (1,)), ((), ())), preferred_element_type=F32)


def gelu_half(pre_act):
    sq = pre_act * pre_act
    t = jnp.tanh(pre_act * (GELU_C + (GELU_C * GELU_K) * sq))
    return sq, t, 0.5 + 0.5 * t


def inv_rms_of(hid_f):
    return lax.rsqrt(jnp.mean(hid_f * hid_f, axis=-1, keepdims=True) + NORM_EPS)


def kernel(dims, w1_hbm, w2_hbm, x_hbm, tgt_hbm, o1_hbm, o2_hbm, r1_hbm, r2_hbm,
           m1, m2, l1, l2, hs, err, acc, tgt, ff, nrm, err_lo, nrm_t, err_t, head_two, st1, st2,
           load_sem, data_sem, stage_sem, out_sem, send_sem, recv_sem):
    n_rows, n_cols, n_steps, n_layers, batch, d_model, d_ff = dims
    f_blk = d_ff // CHUNKS
    n_blk = n_layers * CHUNKS
    n_tiles = batch // TILE
    act, dpre = ff.at[0], ff.at[1]
    pieces = [slice(i, i + SUB) for i in range(0, batch, SUB)]
    row, col = lax.axis_index("row"), lax.axis_index("col")
    peers = ((row, lax.rem(col + 1, n_cols)), (row, lax.rem(col + n_cols - 1, n_cols)), (n_rows - 1 - row, col))

    def cols_of(blk):
        return pl.ds(pl.multiple_of(lax.rem(blk, CHUNKS) * f_blk, f_blk), f_blk)

    def load_copies(blk):
        layer = lax.div(blk, CHUNKS)
        return (pltpu.make_async_copy(w1_hbm.at[layer, :, cols_of(blk)], m1.at[blk], load_sem.at[blk, 0]),
                pltpu.make_async_copy(w2_hbm.at[layer, cols_of(blk), :], m2.at[blk], load_sem.at[blk, 1]))

    def out_copies(blk):
        layer = lax.div(blk, CHUNKS)
        return (pltpu.make_async_copy(m1.at[blk], o1_hbm.at[layer, :, cols_of(blk)], out_sem.at[blk, 0]),
                pltpu.make_async_copy(m2.at[blk], o2_hbm.at[layer, cols_of(blk), :], out_sem.at[blk, 1]))

    def input_copy(step):
        return pltpu.make_async_copy(x_hbm.at[step], hs.at[0], data_sem.at[0])

    def target_copy(step):
        return pltpu.make_async_copy(tgt_hbm.at[step], tgt, data_sem.at[1])

    wires = ((m1, l1, r1_hbm, st1), (m2, l2, r2_hbm, st2))

    def sends(step, blk, mat, src=None):
        out = []
        for slot, peer in enumerate(peers):
            out.append(pltpu.make_async_remote_copy(
                src_ref=wires[mat][1].at[blk] if src is None else src, dst_ref=wires[mat][2].at[step, slot, blk],
                send_sem=send_sem.at[blk, mat, slot], recv_sem=recv_sem.at[step, blk, mat, slot],
                device_id=peer, device_id_type=MESH))
        return out

    def start_sends(step, blk, mat, src=None):
        for cp in sends(step, blk, mat, src):
            cp.start()

    def sent_early(blk):
        layer, chunk = lax.div(blk, CHUNKS), lax.rem(blk, CHUNKS)
        return jnp.logical_and(chunk < CHUNKS - 1, layer > 0)

    def tile_rows(i):
        return pl.ds(pl.multiple_of(i * TILE, TILE), TILE)

    def mix(step, blk, mats=(0, 1)):
        for mat in mats:
            for cp in sends(step, blk, mat):
                cp.wait_recv()
        stage = [pltpu.make_async_copy(wires[mat][2].at[step, slot, blk], wires[mat][3].at[slot], stage_sem.at[mat, slot])
                 for mat in mats for slot in range(3)]
        for cp in stage:
            cp.start()
        for mat in mats:
            for cp in sends(step, blk, mat):
                cp.wait_send()
        for cp in stage:
            cp.wait()
        for mat in mats:
            own, lo, _, st = wires[mat]
            other = st[2].astype(F32)
            new = (own[blk] + st[0].astype(F32) + st[1].astype(F32) + other + other) * 0.2
            own[blk] = new
            lo[blk] = new.astype(BF16)

    barrier = pltpu.get_barrier_semaphore()
    for peer in peers:
        pl.semaphore_signal(barrier, inc=1, device_id=peer, device_id_type=MESH)
    input_copy(0).start()

    for blk in range(CHUNKS):
        for cp in load_copies(blk):
            cp.start()
    target_copy(0).start()

    def first_forward():
        @pl.loop(0, n_layers)
        def _(layer):
            base = layer * CHUNKS

            @pl.when(layer < n_layers - 1)
            def _():
                for c in range(CHUNKS):
                    for cp in load_copies(lax.min(base + CHUNKS + c, n_blk - 1)):
                        cp.start()

            for c in range(CHUNKS):
                for cp in load_copies(base + c):
                    cp.wait()
                l1[base + c] = m1[base + c].astype(BF16)
                l2[base + c] = m2[base + c].astype(BF16)

            behind = None
            for rows in pieces + [None]:
                pre = []
                if rows is not None:
                    hid_f = hs[layer, rows, :].astype(F32)
                    n_lo = (hid_f * inv_rms_of(hid_f)).astype(BF16)
                    nrm[rows, :] = n_lo
                    pre = [matmul(n_lo, l1[base + c]) for c in range(CHUNKS)]
                if behind is not None:
                    b_rows, b_hid, b_act = behind
                    mlp = matmul(b_act[0], l2[base])
                    for c in range(1, CHUNKS):
                        mlp += matmul(b_act[c], l2[base + c])
                    hs[layer + 1, b_rows, :] = (b_hid + mlp).astype(BF16)
                if rows is not None:
                    b_act = [(z * gelu_half(z)[2]).astype(BF16) for z in pre]
                    act[rows, :] = b_act[0]
                    behind = (rows, hid_f, b_act)


    @pl.loop(0, n_steps)
    def _(step):
        input_copy(step).wait()

        @pl.when(step == 0)
        def _():
            first_forward()

        @pl.when(step > 0)
        def _():
            @pl.loop(0, n_blk)
            def _(k):
                blk = n_blk - CHUNKS - CHUNKS * lax.div(k, CHUNKS) + lax.rem(k, CHUNKS)

                @pl.when(sent_early(blk))
                def _():
                    mix(step - 1, blk)

        @pl.loop(0, lax.select(step > 0, n_blk, 0))
        def _(blk):
            layer, chunk = lax.div(blk, CHUNKS), lax.rem(blk, CHUNKS)
            last_blk = blk == n_blk - 1

            @pl.when(chunk == 0)
            def _():
                @pl.loop(0, n_tiles)
                def _(i):
                    rows = tile_rows(i)
                    hid_f = hs[layer, rows, :].astype(F32)
                    n_f = hid_f * inv_rms_of(hid_f)
                    nrm[rows, :] = n_f.astype(BF16)
                    acc[rows, :] = hid_f

            @pl.when(jnp.logical_not(jnp.logical_or(sent_early(blk), last_blk)))
            def _():
                mix(step - 1, blk)

            @pl.when(jnp.logical_not(last_blk))
            def _():
                keep = lax.select(blk == n_blk - CHUNKS, 0, 1)
                behind = None
                for rows in pieces + [None]:
                    if rows is not None:
                        pre = matmul(nrm[rows, :], l1[blk])
                    if behind is not None:
                        acc[behind[0], :] += matmul(behind[1], l2[blk])
                    if rows is not None:
                        a_lo = (pre * gelu_half(pre)[2]).astype(BF16)
                        ff[keep, rows, :] = a_lo
                        behind = (rows, a_lo)

            @pl.when(last_blk)
            def _():
                mix(step - 1, blk, (0,))
                for rows in pieces:
                    pre = matmul(nrm[rows, :], l1[blk])
                    dpre[rows, :] = (pre * gelu_half(pre)[2]).astype(BF16)
                mix(step - 1, blk, (1,))
                for rows in pieces:
                    hs[n_layers, rows, :] = (acc[rows, :] + matmul(dpre[rows, :], l2[blk])).astype(BF16)

            @pl.when(jnp.logical_and(chunk == CHUNKS - 1, layer < n_layers - 1))
            def _():
                @pl.loop(0, n_tiles)
                def _(i):
                    rows = tile_rows(i)
                    hs[layer + 1, rows, :] = acc[rows, :].astype(BF16)

        target_copy(step).wait()

        @pl.loop(0, n_tiles)
        def _(i):
            rows = tile_rows(i)
            hid = hs[n_layers, rows, :].astype(F32)
            e_f = (2.0 / (batch * d_model)) * (hid - tgt[rows, :].astype(F32))
            err[rows, :] = e_f
            err_lo[rows, :] = e_f.astype(BF16)
            err_t[:, rows] = e_f.T.astype(BF16)
            acc[rows, :] = jnp.zeros((TILE, d_model), F32)

        head_blk = n_blk - CHUNKS
        upd_head = m2[head_blk] - LEARN_RATE * matmul(err_t[...], act[...]).T
        m2[head_blk] = upd_head
        head_two[...] = upd_head.astype(BF16)

        @pl.when(step == 0)
        def _():
            pl.semaphore_wait(barrier, 3)

        start_sends(step, head_blk, 1, head_two)

        @pl.loop(0, n_tiles)
        def _(i):
            rows = tile_rows(i)
            nrm_t[:, rows] = nrm[rows, :].astype(F32).T.astype(BF16)

        @pl.loop(0, n_blk)
        def _(k):
            layer, chunk = n_layers - 1 - lax.div(k, CHUNKS), lax.rem(k, CHUNKS)
            blk = layer * CHUNKS + chunk

            @pl.when(jnp.logical_and(chunk == 0, k > 0))
            def _():
                @pl.loop(0, n_tiles)
                def _(i):
                    rows = tile_rows(i)
                    hid_f = hs[layer, rows, :].astype(F32)
                    n_f = hid_f * inv_rms_of(hid_f)
                    nrm[rows, :] = n_f.astype(BF16)
                    nrm_t[:, rows] = n_f.T.astype(BF16)
                    e_f = err[rows, :]
                    err_lo[rows, :] = e_f.astype(BF16)
                    err_t[:, rows] = e_f.T.astype(BF16)
                    acc[rows, :] = jnp.zeros((TILE, d_model), F32)

            @pl.loop(0, n_tiles)
            def _(i):
                rows = tile_rows(i)
                pre = matmul(nrm[rows, :], l1[blk])
                sq, t, half = gelu_half(pre)
                act[rows, :] = (pre * half).astype(BF16)
                slope = half + ((half * (1.0 - t)) * pre) * (GELU_C + (3.0 * GELU_C * GELU_K) * sq)
                d_pre = (matmul_t(err_lo[rows, :], l2[blk]) * slope).astype(BF16)
                dpre[rows, :] = d_pre
                acc[rows, :] += matmul_t(d_pre, l1[blk])

            @pl.when(k > 0)
            def _():
                upd_two = m2[blk] - LEARN_RATE * matmul(err_t[...], act[...]).T
                m2[blk] = upd_two
                l2[blk] = upd_two.astype(BF16)

                @pl.when(sent_early(blk))
                def _():
                    start_sends(step, blk, 1)

            grad_one = matmul(nrm_t[...], dpre[...])
            upd_one = m1[blk] - LEARN_RATE * grad_one
            m1[blk] = upd_one
            l1[blk] = upd_one.astype(BF16)

            @pl.when(sent_early(blk))
            def _():
                start_sends(step, blk, 0)

            @pl.when(jnp.logical_and(chunk == CHUNKS - 1, layer > 0))
            def _():
                @pl.loop(0, n_tiles)
                def _(i):
                    rows = tile_rows(i)
                    hid_f = hs[layer, rows, :].astype(F32)
                    inv = inv_rms_of(hid_f)
                    n_f = hid_f * inv
                    d_n = acc[rows, :]
                    err[rows, :] += inv * (d_n - n_f * jnp.mean(d_n * n_f, axis=-1, keepdims=True))

        @pl.loop(0, n_blk)
        def _(blk):
            @pl.when(jnp.logical_not(sent_early(blk)))
            def _():
                start_sends(step, blk, 0)
                start_sends(step, blk, 1)

        @pl.when(step < n_steps - 1)
        def _():
            input_copy(lax.min(step + 1, n_steps - 1)).start()
            target_copy(lax.min(step + 1, n_steps - 1)).start()

    for early in (True, False):
        @pl.loop(0, n_blk)
        def _(blk):
            turn = sent_early(blk) if early else jnp.logical_not(sent_early(blk))

            @pl.when(turn)
            def _():
                mix(n_steps - 1, blk)
                for cp in out_copies(blk):
                    cp.start()

    @pl.loop(0, n_blk)
    def _(blk):
        for cp in out_copies(blk):
            cp.wait()


def solution(mesh):
    n_rows = mesh.shape['row']
    n_cols = mesh.shape['col']

    def device_fn(w_one, w_two, inputs, targets):
        n_layers, d_model, d_ff = w_one.shape[2:]
        n_steps, batch = inputs.shape[2:4]
        f_blk = d_ff // CHUNKS
        n_blk = n_layers * CHUNKS
        dims = (n_rows, n_cols, n_steps, n_layers, batch, d_model, d_ff)
        any_spec = pl.BlockSpec(memory_space=pl.ANY)
        out = pl.pallas_call(
            functools.partial(kernel, dims),
            out_shape=(
                jax.ShapeDtypeStruct((n_layers, d_model, d_ff), F32),
                jax.ShapeDtypeStruct((n_layers, d_ff, d_model), F32),
                jax.ShapeDtypeStruct((n_steps, 3, n_blk, d_model, f_blk), BF16),
                jax.ShapeDtypeStruct((n_steps, 3, n_blk, f_blk, d_model), BF16),
            ),
            in_specs=[any_spec] * 4,
            out_specs=(any_spec,) * 4,
            scratch_shapes=[
                pltpu.VMEM((n_blk, d_model, f_blk), F32),
                pltpu.VMEM((n_blk, f_blk, d_model), F32),
                pltpu.VMEM((n_blk, d_model, f_blk), BF16),
                pltpu.VMEM((n_blk, f_blk, d_model), BF16),
                pltpu.VMEM((n_layers + 1, batch, d_model), BF16),
                pltpu.VMEM((batch, d_model), F32),
                pltpu.VMEM((batch, d_model), F32),
                pltpu.VMEM((batch, d_model), BF16),
                pltpu.VMEM((2, batch, f_blk), BF16),
                pltpu.VMEM((batch, d_model), BF16),
                pltpu.VMEM((batch, d_model), BF16),
                pltpu.VMEM((d_model, batch), BF16),
                pltpu.VMEM((d_model, batch), BF16),
                pltpu.VMEM((f_blk, d_model), BF16),
                pltpu.VMEM((3, d_model, f_blk), BF16),
                pltpu.VMEM((3, f_blk, d_model), BF16),
                pltpu.SemaphoreType.DMA((n_blk, 2)),
                pltpu.SemaphoreType.DMA((2,)),
                pltpu.SemaphoreType.DMA((2, 3)),
                pltpu.SemaphoreType.DMA((n_blk, 2)),
                pltpu.SemaphoreType.DMA((n_blk, 2, 3)),
                pltpu.SemaphoreType.DMA((n_steps, n_blk, 2, 3)),
            ],
            compiler_params=pltpu.CompilerParams(
                collective_id=0, has_side_effects=True, vmem_limit_bytes=67_043_328),
            name="gossip_sgd",
        )(w_one[0, 0], w_two[0, 0], inputs[0, 0], targets[0, 0])
        return out[0][None, None], out[1][None, None]

    grid_spec = P('row', 'col')
    return jax.shard_map(device_fn, mesh=mesh, in_specs=(grid_spec,) * 4, out_specs=(grid_spec, grid_spec), check_vma=False)
```

```python
import functools

import jax
import jax.numpy as jnp
from jax import lax
from jax.experimental import pallas as pl
from jax.experimental.pallas import tpu as pltpu
from jax.sharding import PartitionSpec as P

LEARN_RATE = 1.5
NORM_EPS = 1e-6
GELU_C = 0.7978845608028654
GELU_K = 0.044715

MESH = pl.DeviceIdType.MESH
F32 = jnp.float32
BF16 = jnp.bfloat16
CHUNKS = 3
TILE = 512
SUB = 256


def matmul(lhs, rhs):
    return jnp.dot(lhs, rhs, preferred_element_type=F32)


def matmul_t(lhs, rhs):
    return lax.dot_general(lhs, rhs, (((1,), (1,)), ((), ())), preferred_element_type=F32)


def gelu_half(pre_act):
    sq = pre_act * pre_act
    t = jnp.tanh(pre_act * (GELU_C + (GELU_C * GELU_K) * sq))
    return sq, t, 0.5 + 0.5 * t


def inv_rms_of(hid_f):
    return lax.rsqrt(jnp.mean(hid_f * hid_f, axis=-1, keepdims=True) + NORM_EPS)


def kernel(dims, w1_hbm, w2_hbm, x_hbm, tgt_hbm, o1_hbm, o2_hbm, r1_hbm, r2_hbm,
           m1, m2, l1, l2, hs, err, acc, tgt, ff, nrm, err_lo, nrm_t, err_t, head_two, st1, st2,
           load_sem, data_sem, stage_sem, out_sem, send_sem, recv_sem):
    n_rows, n_cols, n_steps, n_layers, batch, d_model, d_ff = dims
    f_blk = d_ff // CHUNKS
    n_blk = n_layers * CHUNKS
    n_tiles = batch // TILE
    act, dpre = ff.at[0], ff.at[1]
    pieces = [slice(i, i + SUB) for i in range(0, batch, SUB)]
    row, col = lax.axis_index("row"), lax.axis_index("col")
    peers = ((row, lax.rem(col + 1, n_cols)), (row, lax.rem(col + n_cols - 1, n_cols)), (n_rows - 1 - row, col))

    def cols_of(blk):
        return pl.ds(pl.multiple_of(lax.rem(blk, CHUNKS) * f_blk, f_blk), f_blk)

    def load_copies(blk):
        layer = lax.div(blk, CHUNKS)
        return (pltpu.make_async_copy(w1_hbm.at[layer, :, cols_of(blk)], m1.at[blk], load_sem.at[blk, 0]),
                pltpu.make_async_copy(w2_hbm.at[layer, cols_of(blk), :], m2.at[blk], load_sem.at[blk, 1]))

    def out_copy(blk, mat):
        layer = lax.div(blk, CHUNKS)
        if mat == 0:
            return pltpu.make_async_copy(m1.at[blk], o1_hbm.at[layer, :, cols_of(blk)], out_sem.at[blk, 0])
        return pltpu.make_async_copy(m2.at[blk], o2_hbm.at[layer, cols_of(blk), :], out_sem.at[blk, 1])

    def input_copy(step):
        return pltpu.make_async_copy(x_hbm.at[step], hs.at[0], data_sem.at[0])

    def target_copy(step):
        return pltpu.make_async_copy(tgt_hbm.at[step], tgt, data_sem.at[1])

    wires = ((m1, l1, r1_hbm, st1), (m2, l2, r2_hbm, st2))

    def sends(step, blk, mat, src=None):
        out = []
        for slot, peer in enumerate(peers):
            out.append(pltpu.make_async_remote_copy(
                src_ref=wires[mat][1].at[blk] if src is None else src, dst_ref=wires[mat][2].at[step, slot, blk],
                send_sem=send_sem.at[blk, mat, slot], recv_sem=recv_sem.at[step, blk, mat, slot],
                device_id=peer, device_id_type=MESH))
        return out

    def start_sends(step, blk, mat, src=None):
        for cp in sends(step, blk, mat, src):
            cp.start()

    def sent_early(blk):
        layer, chunk = lax.div(blk, CHUNKS), lax.rem(blk, CHUNKS)
        return jnp.logical_and(chunk < CHUNKS - 1, layer > 0)

    def tile_rows(i):
        return pl.ds(pl.multiple_of(i * TILE, TILE), TILE)

    def mix(step, blk, mats=(0, 1)):
        for mat in mats:
            for cp in sends(step, blk, mat):
                cp.wait_recv()
        stage = [pltpu.make_async_copy(wires[mat][2].at[step, slot, blk], wires[mat][3].at[slot], stage_sem.at[mat, slot])
                 for mat in mats for slot in range(3)]
        for cp in stage:
            cp.start()
        for mat in mats:
            for cp in sends(step, blk, mat):
                cp.wait_send()
        for cp in stage:
            cp.wait()
        for mat in mats:
            own, lo, _, st = wires[mat]
            other = st[2].astype(F32)
            new = (own[blk] + st[0].astype(F32) + st[1].astype(F32) + other + other) * 0.2
            own[blk] = new
            lo[blk] = new.astype(BF16)

    barrier = pltpu.get_barrier_semaphore()
    for peer in peers:
        pl.semaphore_signal(barrier, inc=1, device_id=peer, device_id_type=MESH)
    input_copy(0).start()

    for blk in range(CHUNKS):
        for cp in load_copies(blk):
            cp.start()
    target_copy(0).start()

    def first_forward():
        @pl.loop(0, n_layers)
        def _(layer):
            base = layer * CHUNKS

            @pl.when(layer < n_layers - 1)
            def _():
                for c in range(CHUNKS):
                    for cp in load_copies(lax.min(base + CHUNKS + c, n_blk - 1)):
                        cp.start()

            for c in range(CHUNKS):
                for cp in load_copies(base + c):
                    cp.wait()
                l1[base + c] = m1[base + c].astype(BF16)
                l2[base + c] = m2[base + c].astype(BF16)

            behind = None
            for rows in pieces + [None]:
                pre = []
                if rows is not None:
                    hid_f = hs[layer, rows, :].astype(F32)
                    n_lo = (hid_f * inv_rms_of(hid_f)).astype(BF16)
                    nrm[rows, :] = n_lo
                    pre = [matmul(n_lo, l1[base + c]) for c in range(CHUNKS)]
                if behind is not None:
                    b_rows, b_hid, b_act = behind
                    mlp = matmul(b_act[0], l2[base])
                    for c in range(1, CHUNKS):
                        mlp += matmul(b_act[c], l2[base + c])
                    hs[layer + 1, b_rows, :] = (b_hid + mlp).astype(BF16)
                if rows is not None:
                    b_act = [(z * gelu_half(z)[2]).astype(BF16) for z in pre]
                    act[rows, :] = b_act[0]
                    behind = (rows, hid_f, b_act)


    @pl.loop(0, n_steps)
    def _(step):
        input_copy(step).wait()

        @pl.when(step == 0)
        def _():
            first_forward()

        @pl.when(step > 0)
        def _():
            @pl.loop(0, n_blk)
            def _(k):
                blk = n_blk - CHUNKS - CHUNKS * lax.div(k, CHUNKS) + lax.rem(k, CHUNKS)

                @pl.when(sent_early(blk))
                def _():
                    mix(step - 1, blk)

        @pl.loop(0, lax.select(step > 0, n_blk, 0))
        def _(blk):
            layer, chunk = lax.div(blk, CHUNKS), lax.rem(blk, CHUNKS)
            last_blk = blk == n_blk - 1

            @pl.when(chunk == 0)
            def _():
                @pl.loop(0, n_tiles)
                def _(i):
                    rows = tile_rows(i)
                    hid_f = hs[layer, rows, :].astype(F32)
                    n_f = hid_f * inv_rms_of(hid_f)
                    nrm[rows, :] = n_f.astype(BF16)
                    acc[rows, :] = hid_f

            @pl.when(jnp.logical_not(jnp.logical_or(sent_early(blk), last_blk)))
            def _():
                mix(step - 1, blk)

            @pl.when(jnp.logical_not(last_blk))
            def _():
                keep = lax.select(blk == n_blk - CHUNKS, 0, 1)
                behind = None
                for rows in pieces + [None]:
                    if rows is not None:
                        pre = matmul(nrm[rows, :], l1[blk])
                    if behind is not None:
                        acc[behind[0], :] += matmul(behind[1], l2[blk])
                    if rows is not None:
                        a_lo = (pre * gelu_half(pre)[2]).astype(BF16)
                        ff[keep, rows, :] = a_lo
                        behind = (rows, a_lo)

            @pl.when(last_blk)
            def _():
                mix(step - 1, blk, (0,))
                for rows in pieces:
                    pre = matmul(nrm[rows, :], l1[blk])
                    dpre[rows, :] = (pre * gelu_half(pre)[2]).astype(BF16)
                mix(step - 1, blk, (1,))
                for rows in pieces:
                    hs[n_layers, rows, :] = (acc[rows, :] + matmul(dpre[rows, :], l2[blk])).astype(BF16)

            @pl.when(jnp.logical_and(chunk == CHUNKS - 1, layer < n_layers - 1))
            def _():
                @pl.loop(0, n_tiles)
                def _(i):
                    rows = tile_rows(i)
                    hs[layer + 1, rows, :] = acc[rows, :].astype(BF16)

        target_copy(step).wait()

        @pl.loop(0, n_tiles)
        def _(i):
            rows = tile_rows(i)
            hid = hs[n_layers, rows, :].astype(F32)
            e_f = (2.0 / (batch * d_model)) * (hid - tgt[rows, :].astype(F32))
            err[rows, :] = e_f
            err_lo[rows, :] = e_f.astype(BF16)
            err_t[:, rows] = e_f.T.astype(BF16)
            acc[rows, :] = jnp.zeros((TILE, d_model), F32)

        head_blk = n_blk - CHUNKS
        upd_head = m2[head_blk] - LEARN_RATE * matmul(err_t[...], act[...]).T
        m2[head_blk] = upd_head
        head_two[...] = upd_head.astype(BF16)

        @pl.when(step == 0)
        def _():
            pl.semaphore_wait(barrier, 3)

        at_once = jnp.logical_or(step > 0, lax.rem(row + col, 2) == 0)

        @pl.when(at_once)
        def _():
            start_sends(step, head_blk, 1, head_two)

        @pl.loop(0, n_tiles)
        def _(i):
            rows = tile_rows(i)
            nrm_t[:, rows] = nrm[rows, :].astype(F32).T.astype(BF16)

        @pl.loop(0, n_blk)
        def _(k):
            layer, chunk = n_layers - 1 - lax.div(k, CHUNKS), lax.rem(k, CHUNKS)
            blk = layer * CHUNKS + chunk

            @pl.when(jnp.logical_and(chunk == 0, k > 0))
            def _():
                @pl.loop(0, n_tiles)
                def _(i):
                    rows = tile_rows(i)
                    hid_f = hs[layer, rows, :].astype(F32)
                    n_f = hid_f * inv_rms_of(hid_f)
                    nrm[rows, :] = n_f.astype(BF16)
                    nrm_t[:, rows] = n_f.T.astype(BF16)
                    e_f = err[rows, :]
                    err_lo[rows, :] = e_f.astype(BF16)
                    err_t[:, rows] = e_f.T.astype(BF16)
                    acc[rows, :] = jnp.zeros((TILE, d_model), F32)

            @pl.loop(0, n_tiles)
            def _(i):
                rows = tile_rows(i)
                pre = matmul(nrm[rows, :], l1[blk])
                sq, t, half = gelu_half(pre)
                act[rows, :] = (pre * half).astype(BF16)
                slope = half + ((half * (1.0 - t)) * pre) * (GELU_C + (3.0 * GELU_C * GELU_K) * sq)
                d_pre = (matmul_t(err_lo[rows, :], l2[blk]) * slope).astype(BF16)
                dpre[rows, :] = d_pre
                acc[rows, :] += matmul_t(d_pre, l1[blk])

            @pl.when(k > 0)
            def _():
                upd_two = m2[blk] - LEARN_RATE * matmul(err_t[...], act[...]).T
                m2[blk] = upd_two
                l2[blk] = upd_two.astype(BF16)

                @pl.when(sent_early(blk))
                def _():
                    start_sends(step, blk, 1)

            grad_one = matmul(nrm_t[...], dpre[...])
            upd_one = m1[blk] - LEARN_RATE * grad_one
            m1[blk] = upd_one
            l1[blk] = upd_one.astype(BF16)

            @pl.when(jnp.logical_and(k == 0, jnp.logical_not(at_once)))
            def _():
                start_sends(step, head_blk, 1, head_two)

            @pl.when(sent_early(blk))
            def _():
                start_sends(step, blk, 0)

            @pl.when(jnp.logical_and(chunk == CHUNKS - 1, layer > 0))
            def _():
                @pl.loop(0, n_tiles)
                def _(i):
                    rows = tile_rows(i)
                    hid_f = hs[layer, rows, :].astype(F32)
                    inv = inv_rms_of(hid_f)
                    n_f = hid_f * inv
                    d_n = acc[rows, :]
                    err[rows, :] += inv * (d_n - n_f * jnp.mean(d_n * n_f, axis=-1, keepdims=True))

        @pl.loop(0, n_blk)
        def _(blk):
            @pl.when(jnp.logical_not(sent_early(blk)))
            def _():
                start_sends(step, blk, 0)
                start_sends(step, blk, 1)

        @pl.when(step < n_steps - 1)
        def _():
            input_copy(lax.min(step + 1, n_steps - 1)).start()
            target_copy(lax.min(step + 1, n_steps - 1)).start()

    for early in (True, False):
        @pl.loop(0, n_blk)
        def _(blk):
            turn = sent_early(blk) if early else jnp.logical_not(sent_early(blk))

            @pl.when(turn)
            def _():
                for mat in range(2):
                    mix(n_steps - 1, blk, (mat,))
                    out_copy(blk, mat).start()

    @pl.loop(0, n_blk)
    def _(blk):
        for mat in range(2):
            out_copy(blk, mat).wait()


def solution(mesh):
    n_rows = mesh.shape['row']
    n_cols = mesh.shape['col']

    def device_fn(w_one, w_two, inputs, targets):
        n_layers, d_model, d_ff = w_one.shape[2:]
        n_steps, batch = inputs.shape[2:4]
        f_blk = d_ff // CHUNKS
        n_blk = n_layers * CHUNKS
        dims = (n_rows, n_cols, n_steps, n_layers, batch, d_model, d_ff)
        any_spec = pl.BlockSpec(memory_space=pl.ANY)
        out = pl.pallas_call(
            functools.partial(kernel, dims),
            out_shape=(
                jax.ShapeDtypeStruct((n_layers, d_model, d_ff), F32),
                jax.ShapeDtypeStruct((n_layers, d_ff, d_model), F32),
                jax.ShapeDtypeStruct((n_steps, 3, n_blk, d_model, f_blk), BF16),
                jax.ShapeDtypeStruct((n_steps, 3, n_blk, f_blk, d_model), BF16),
            ),
            in_specs=[any_spec] * 4,
            out_specs=(any_spec,) * 4,
            scratch_shapes=[
                pltpu.VMEM((n_blk, d_model, f_blk), F32),
                pltpu.VMEM((n_blk, f_blk, d_model), F32),
                pltpu.VMEM((n_blk, d_model, f_blk), BF16),
                pltpu.VMEM((n_blk, f_blk, d_model), BF16),
                pltpu.VMEM((n_layers + 1, batch, d_model), BF16),
                pltpu.VMEM((batch, d_model), F32),
                pltpu.VMEM((batch, d_model), F32),
                pltpu.VMEM((batch, d_model), BF16),
                pltpu.VMEM((2, batch, f_blk), BF16),
                pltpu.VMEM((batch, d_model), BF16),
                pltpu.VMEM((batch, d_model), BF16),
                pltpu.VMEM((d_model, batch), BF16),
                pltpu.VMEM((d_model, batch), BF16),
                pltpu.VMEM((f_blk, d_model), BF16),
                pltpu.VMEM((3, d_model, f_blk), BF16),
                pltpu.VMEM((3, f_blk, d_model), BF16),
                pltpu.SemaphoreType.DMA((n_blk, 2)),
                pltpu.SemaphoreType.DMA((2,)),
                pltpu.SemaphoreType.DMA((2, 3)),
                pltpu.SemaphoreType.DMA((n_blk, 2)),
                pltpu.SemaphoreType.DMA((n_blk, 2, 3)),
                pltpu.SemaphoreType.DMA((n_steps, n_blk, 2, 3)),
            ],
            compiler_params=pltpu.CompilerParams(
                collective_id=0, has_side_effects=True, vmem_limit_bytes=67_043_328),
            name="gossip_sgd",
        )(w_one[0, 0], w_two[0, 0], inputs[0, 0], targets[0, 0])
        return out[0][None, None], out[1][None, None]

    grid_spec = P('row', 'col')
    return jax.shard_map(device_fn, mesh=mesh, in_specs=(grid_spec,) * 4, out_specs=(grid_spec, grid_spec), check_vma=False)
```

```python
import functools

import jax
import jax.numpy as jnp
from jax import lax
from jax.experimental import pallas as pl
from jax.experimental.pallas import tpu as pltpu
from jax.sharding import PartitionSpec as P

LEARN_RATE = 1.5
NORM_EPS = 1e-6
GELU_C = 0.7978845608028654
GELU_K = 0.044715

MESH = pl.DeviceIdType.MESH
F32 = jnp.float32
BF16 = jnp.bfloat16
CHUNKS = 3
TILE = 512
VMEM_BYTES = 47_000_000
SUB = 256


def matmul(lhs, rhs):
    return jnp.dot(lhs, rhs, preferred_element_type=F32)


def matmul_t(lhs, rhs):
    return lax.dot_general(lhs, rhs, (((1,), (1,)), ((), ())), preferred_element_type=F32)


def gelu_half(pre_act):
    sq = pre_act * pre_act
    t = jnp.tanh(pre_act * (GELU_C + (GELU_C * GELU_K) * sq))
    return sq, t, 0.5 + 0.5 * t


def inv_rms_of(hid_f):
    return lax.rsqrt(jnp.mean(hid_f * hid_f, axis=-1, keepdims=True) + NORM_EPS)


def kernel(dims, w1_hbm, w2_hbm, x_hbm, tgt_hbm, m1, m2, r1_hbm, r2_hbm,
           l1, l2, hs, err, acc, tgt, ff, nrm, err_lo, nrm_t, err_t, head_two, st1, st2,
           load_sem, data_sem, stage_sem, send_sem, recv_sem):
    n_rows, n_cols, n_steps, n_layers, batch, d_model, d_ff = dims
    f_blk = d_ff // CHUNKS
    n_blk = n_layers * CHUNKS
    n_tiles = batch // TILE
    act, dpre = ff.at[0], ff.at[1]
    pieces = [slice(i, i + SUB) for i in range(0, batch, SUB)]
    row, col = lax.axis_index("row"), lax.axis_index("col")
    peers = ((row, lax.rem(col + 1, n_cols)), (row, lax.rem(col + n_cols - 1, n_cols)), (n_rows - 1 - row, col))

    def cols_of(blk):
        return pl.ds(pl.multiple_of(lax.rem(blk, CHUNKS) * f_blk, f_blk), f_blk)

    def load_copies(blk):
        layer = lax.div(blk, CHUNKS)
        return (pltpu.make_async_copy(w1_hbm.at[layer, :, cols_of(blk)], m1.at[layer, :, cols_of(blk)], load_sem.at[blk, 0]),
                pltpu.make_async_copy(w2_hbm.at[layer, cols_of(blk), :], m2.at[blk], load_sem.at[blk, 1]))

    def input_copy(step):
        return pltpu.make_async_copy(x_hbm.at[step], hs.at[0], data_sem.at[0])

    def target_copy(step):
        return pltpu.make_async_copy(tgt_hbm.at[step], tgt, data_sem.at[1])

    wires = ((None, l1, r1_hbm, st1), (None, l2, r2_hbm, st2))

    def sends(step, blk, mat, src=None):
        out = []
        for slot, peer in enumerate(peers):
            out.append(pltpu.make_async_remote_copy(
                src_ref=wires[mat][1].at[blk] if src is None else src, dst_ref=wires[mat][2].at[step, slot, blk],
                send_sem=send_sem.at[blk, mat, slot], recv_sem=recv_sem.at[step, blk, mat, slot],
                device_id=peer, device_id_type=MESH))
        return out

    def start_sends(step, blk, mat, src=None):
        for cp in sends(step, blk, mat, src):
            cp.start()

    def sent_early(blk):
        layer, chunk = lax.div(blk, CHUNKS), lax.rem(blk, CHUNKS)
        return jnp.logical_and(chunk < CHUNKS - 1, layer > 0)

    def tile_rows(i):
        return pl.ds(pl.multiple_of(i * TILE, TILE), TILE)

    def mix(step, blk, mats=(0, 1)):
        for mat in mats:
            for cp in sends(step, blk, mat):
                cp.wait_recv()
        stage = [pltpu.make_async_copy(wires[mat][2].at[step, slot, blk], wires[mat][3].at[slot], stage_sem.at[mat, slot])
                 for mat in mats for slot in range(3)]
        for cp in stage:
            cp.start()
        for mat in mats:
            for cp in sends(step, blk, mat):
                cp.wait_send()
        for cp in stage:
            cp.wait()
        for mat in mats:
            _, lo, _, st = wires[mat]
            own, at = (m1, (lax.div(blk, CHUNKS), slice(None), cols_of(blk))) if mat == 0 else (m2, (blk,))
            other = st[2].astype(F32)
            new = (own[at] + st[0].astype(F32) + st[1].astype(F32) + other + other) * 0.2
            own[at] = new
            lo[blk] = new.astype(BF16)

    barrier = pltpu.get_barrier_semaphore()
    for peer in peers:
        pl.semaphore_signal(barrier, inc=1, device_id=peer, device_id_type=MESH)
    input_copy(0).start()

    for blk in range(CHUNKS):
        for cp in load_copies(blk):
            cp.start()
    target_copy(0).start()

    def first_forward():
        @pl.loop(0, n_layers)
        def _(layer):
            base = layer * CHUNKS

            @pl.when(layer < n_layers - 1)
            def _():
                for c in range(CHUNKS):
                    for cp in load_copies(lax.min(base + CHUNKS + c, n_blk - 1)):
                        cp.start()

            for c in range(CHUNKS):
                for cp in load_copies(base + c):
                    cp.wait()
                l1[base + c] = m1[layer, :, c * f_blk:(c + 1) * f_blk].astype(BF16)
                l2[base + c] = m2[base + c].astype(BF16)

            behind = None
            for rows in pieces + [None]:
                pre = []
                if rows is not None:
                    hid_f = hs[layer, rows, :].astype(F32)
                    n_lo = (hid_f * inv_rms_of(hid_f)).astype(BF16)
                    nrm[rows, :] = n_lo
                    pre = [matmul(n_lo, l1[base + c]) for c in range(CHUNKS)]
                if behind is not None:
                    b_rows, b_hid, b_act = behind
                    mlp = matmul(b_act[0], l2[base])
                    for c in range(1, CHUNKS):
                        mlp += matmul(b_act[c], l2[base + c])
                    hs[layer + 1, b_rows, :] = (b_hid + mlp).astype(BF16)
                if rows is not None:
                    b_act = [(z * gelu_half(z)[2]).astype(BF16) for z in pre]
                    act[rows, :] = b_act[0]
                    behind = (rows, hid_f, b_act)


    @pl.loop(0, n_steps)
    def _(step):
        input_copy(step).wait()

        @pl.when(step == 0)
        def _():
            first_forward()

        @pl.when(step > 0)
        def _():
            @pl.loop(0, n_blk)
            def _(k):
                blk = n_blk - CHUNKS - CHUNKS * lax.div(k, CHUNKS) + lax.rem(k, CHUNKS)

                @pl.when(sent_early(blk))
                def _():
                    mix(step - 1, blk)

        @pl.loop(0, lax.select(step > 0, n_blk, 0))
        def _(blk):
            layer, chunk = lax.div(blk, CHUNKS), lax.rem(blk, CHUNKS)
            last_blk = blk == n_blk - 1

            @pl.when(chunk == 0)
            def _():
                @pl.loop(0, n_tiles)
                def _(i):
                    rows = tile_rows(i)
                    hid_f = hs[layer, rows, :].astype(F32)
                    n_f = hid_f * inv_rms_of(hid_f)
                    nrm[rows, :] = n_f.astype(BF16)
                    acc[rows, :] = hid_f

            @pl.when(jnp.logical_not(jnp.logical_or(sent_early(blk), last_blk)))
            def _():
                mix(step - 1, blk)

            @pl.when(jnp.logical_not(last_blk))
            def _():
                keep = lax.select(blk == n_blk - CHUNKS, 0, 1)
                behind = None
                for rows in pieces + [None]:
                    if rows is not None:
                        pre = matmul(nrm[rows, :], l1[blk])
                    if behind is not None:
                        acc[behind[0], :] += matmul(behind[1], l2[blk])
                    if rows is not None:
                        a_lo = (pre * gelu_half(pre)[2]).astype(BF16)
                        ff[keep, rows, :] = a_lo
                        behind = (rows, a_lo)

            @pl.when(last_blk)
            def _():
                mix(step - 1, blk, (0,))
                for rows in pieces:
                    pre = matmul(nrm[rows, :], l1[blk])
                    dpre[rows, :] = (pre * gelu_half(pre)[2]).astype(BF16)
                mix(step - 1, blk, (1,))
                for rows in pieces:
                    hs[n_layers, rows, :] = (acc[rows, :] + matmul(dpre[rows, :], l2[blk])).astype(BF16)

            @pl.when(jnp.logical_and(chunk == CHUNKS - 1, layer < n_layers - 1))
            def _():
                @pl.loop(0, n_tiles)
                def _(i):
                    rows = tile_rows(i)
                    hs[layer + 1, rows, :] = acc[rows, :].astype(BF16)

        target_copy(step).wait()

        @pl.loop(0, n_tiles)
        def _(i):
            rows = tile_rows(i)
            hid = hs[n_layers, rows, :].astype(F32)
            e_f = (2.0 / (batch * d_model)) * (hid - tgt[rows, :].astype(F32))
            err[rows, :] = e_f
            err_lo[rows, :] = e_f.astype(BF16)
            err_t[:, rows] = e_f.T.astype(BF16)
            acc[rows, :] = jnp.zeros((TILE, d_model), F32)

        head_blk = n_blk - CHUNKS
        upd_head = m2[head_blk] - LEARN_RATE * matmul(err_t[...], act[...]).T
        m2[head_blk] = upd_head
        head_two[...] = upd_head.astype(BF16)

        @pl.when(step == 0)
        def _():
            pl.semaphore_wait(barrier, 3)

        at_once = jnp.logical_or(step > 0, lax.rem(row + col, 2) == 0)

        @pl.when(at_once)
        def _():
            start_sends(step, head_blk, 1, head_two)

        @pl.loop(0, n_tiles)
        def _(i):
            rows = tile_rows(i)
            nrm_t[:, rows] = nrm[rows, :].astype(F32).T.astype(BF16)

        @pl.loop(0, n_blk)
        def _(k):
            layer, chunk = n_layers - 1 - lax.div(k, CHUNKS), lax.rem(k, CHUNKS)
            blk = layer * CHUNKS + chunk

            @pl.when(jnp.logical_and(chunk == 0, k > 0))
            def _():
                @pl.loop(0, n_tiles)
                def _(i):
                    rows = tile_rows(i)
                    hid_f = hs[layer, rows, :].astype(F32)
                    n_f = hid_f * inv_rms_of(hid_f)
                    nrm[rows, :] = n_f.astype(BF16)
                    nrm_t[:, rows] = n_f.T.astype(BF16)
                    e_f = err[rows, :]
                    err_lo[rows, :] = e_f.astype(BF16)
                    err_t[:, rows] = e_f.T.astype(BF16)
                    acc[rows, :] = jnp.zeros((TILE, d_model), F32)

            @pl.loop(0, n_tiles)
            def _(i):
                rows = tile_rows(i)
                pre = matmul(nrm[rows, :], l1[blk])
                sq, t, half = gelu_half(pre)
                act[rows, :] = (pre * half).astype(BF16)
                slope = half + ((half * (1.0 - t)) * pre) * (GELU_C + (3.0 * GELU_C * GELU_K) * sq)
                d_pre = (matmul_t(err_lo[rows, :], l2[blk]) * slope).astype(BF16)
                dpre[rows, :] = d_pre
                acc[rows, :] += matmul_t(d_pre, l1[blk])

            @pl.when(k > 0)
            def _():
                upd_two = m2[blk] - LEARN_RATE * matmul(err_t[...], act[...]).T
                m2[blk] = upd_two
                l2[blk] = upd_two.astype(BF16)

                @pl.when(sent_early(blk))
                def _():
                    start_sends(step, blk, 1)

            grad_one = matmul(nrm_t[...], dpre[...])
            upd_one = m1[layer, :, cols_of(blk)] - LEARN_RATE * grad_one
            m1[layer, :, cols_of(blk)] = upd_one
            l1[blk] = upd_one.astype(BF16)

            @pl.when(jnp.logical_and(k == 0, jnp.logical_not(at_once)))
            def _():
                start_sends(step, head_blk, 1, head_two)

            @pl.when(sent_early(blk))
            def _():
                start_sends(step, blk, 0)

            @pl.when(jnp.logical_and(chunk == CHUNKS - 1, layer > 0))
            def _():
                @pl.loop(0, n_tiles)
                def _(i):
                    rows = tile_rows(i)
                    hid_f = hs[layer, rows, :].astype(F32)
                    inv = inv_rms_of(hid_f)
                    n_f = hid_f * inv
                    d_n = acc[rows, :]
                    err[rows, :] += inv * (d_n - n_f * jnp.mean(d_n * n_f, axis=-1, keepdims=True))

        @pl.loop(0, n_blk)
        def _(blk):
            @pl.when(jnp.logical_not(sent_early(blk)))
            def _():
                start_sends(step, blk, 0)
                start_sends(step, blk, 1)

        @pl.when(step < n_steps - 1)
        def _():
            input_copy(lax.min(step + 1, n_steps - 1)).start()
            target_copy(lax.min(step + 1, n_steps - 1)).start()

    for early in (True, False):
        @pl.loop(0, n_blk)
        def _(blk):
            turn = sent_early(blk) if early else jnp.logical_not(sent_early(blk))

            @pl.when(turn)
            def _():
                for mat in range(2):
                    mix(n_steps - 1, blk, (mat,))


def solution(mesh):
    n_rows = mesh.shape['row']
    n_cols = mesh.shape['col']

    def device_fn(w_one, w_two, inputs, targets):
        n_layers, d_model, d_ff = w_one.shape[2:]
        n_steps, batch = inputs.shape[2:4]
        f_blk = d_ff // CHUNKS
        n_blk = n_layers * CHUNKS
        dims = (n_rows, n_cols, n_steps, n_layers, batch, d_model, d_ff)
        any_spec = pl.BlockSpec(memory_space=pl.ANY)
        vmem_spec = pl.BlockSpec(memory_space=pltpu.VMEM)
        out = pl.pallas_call(
            functools.partial(kernel, dims),
            out_shape=(
                pltpu.VMEM((n_layers, d_model, d_ff), F32),
                pltpu.VMEM((n_blk, f_blk, d_model), F32),
                jax.ShapeDtypeStruct((n_steps, 3, n_blk, d_model, f_blk), BF16),
                jax.ShapeDtypeStruct((n_steps, 3, n_blk, f_blk, d_model), BF16),
            ),
            in_specs=[any_spec] * 4,
            out_specs=(vmem_spec, vmem_spec, any_spec, any_spec),
            scratch_shapes=[
                pltpu.VMEM((n_blk, d_model, f_blk), BF16),
                pltpu.VMEM((n_blk, f_blk, d_model), BF16),
                pltpu.VMEM((n_layers + 1, batch, d_model), BF16),
                pltpu.VMEM((batch, d_model), F32),
                pltpu.VMEM((batch, d_model), F32),
                pltpu.VMEM((batch, d_model), BF16),
                pltpu.VMEM((2, batch, f_blk), BF16),
                pltpu.VMEM((batch, d_model), BF16),
                pltpu.VMEM((batch, d_model), BF16),
                pltpu.VMEM((d_model, batch), BF16),
                pltpu.VMEM((d_model, batch), BF16),
                pltpu.VMEM((f_blk, d_model), BF16),
                pltpu.VMEM((3, d_model, f_blk), BF16),
                pltpu.VMEM((3, f_blk, d_model), BF16),
                pltpu.SemaphoreType.DMA((n_blk, 2)),
                pltpu.SemaphoreType.DMA((2,)),
                pltpu.SemaphoreType.DMA((2, 3)),
                pltpu.SemaphoreType.DMA((n_blk, 2, 3)),
                pltpu.SemaphoreType.DMA((n_steps, n_blk, 2, 3)),
            ],
            compiler_params=pltpu.CompilerParams(
                collective_id=0, has_side_effects=True, vmem_limit_bytes=VMEM_BYTES),
            name="gossip_sgd",
        )(w_one[0, 0], w_two[0, 0], inputs[0, 0], targets[0, 0])
        return out[0][None, None], out[1].reshape(w_two.shape)

    grid_spec = P('row', 'col')
    return jax.shard_map(device_fn, mesh=mesh, in_specs=(grid_spec,) * 4, out_specs=(grid_spec, grid_spec), check_vma=False)
```

```python
import functools

import jax
import jax.numpy as jnp
from jax import lax
from jax.experimental import pallas as pl
from jax.experimental.pallas import tpu as pltpu
from jax.sharding import PartitionSpec as P

LEARN_RATE = 1.5
NORM_EPS = 1e-6
GELU_C = 0.7978845608028654
GELU_K = 0.044715

MESH = pl.DeviceIdType.MESH
F32 = jnp.float32
BF16 = jnp.bfloat16
CHUNKS = 3
TILE = 512
VMEM_BYTES = 47_000_000
SUB = 256


def matmul(lhs, rhs):
    return jnp.dot(lhs, rhs, preferred_element_type=F32)


def matmul_t(lhs, rhs):
    return lax.dot_general(lhs, rhs, (((1,), (1,)), ((), ())), preferred_element_type=F32)


def gelu_half(pre_act):
    sq = pre_act * pre_act
    t = jnp.tanh(pre_act * (GELU_C + (GELU_C * GELU_K) * sq))
    return sq, t, 0.5 + 0.5 * t


def inv_rms_of(hid_f):
    return lax.rsqrt(jnp.mean(hid_f * hid_f, axis=-1, keepdims=True) + NORM_EPS)


def kernel(dims, w1_hbm, w2_hbm, x_hbm, tgt_hbm, m1, m2, r1_hbm, r2_hbm,
           l1, l2, hs, err, acc, tgt, ff, nrm, err_lo, nrm_t, err_t, head_two, tail_one, tail_two, st1, st2,
           load_sem, data_sem, stage_sem, send_sem, recv_sem):
    n_rows, n_cols, n_steps, n_layers, batch, d_model, d_ff = dims
    f_blk = d_ff // CHUNKS
    n_blk = n_layers * CHUNKS
    n_tiles = batch // TILE
    act, dpre = ff.at[0], ff.at[1]
    pieces = [slice(i, i + SUB) for i in range(0, batch, SUB)]
    row, col = lax.axis_index("row"), lax.axis_index("col")
    peers = ((row, lax.rem(col + 1, n_cols)), (row, lax.rem(col + n_cols - 1, n_cols)), (n_rows - 1 - row, col))

    def cols_of(blk):
        return pl.ds(pl.multiple_of(lax.rem(blk, CHUNKS) * f_blk, f_blk), f_blk)

    def load_copies(blk):
        layer = lax.div(blk, CHUNKS)
        return (pltpu.make_async_copy(w1_hbm.at[layer, :, cols_of(blk)], m1.at[layer, :, cols_of(blk)], load_sem.at[blk, 0]),
                pltpu.make_async_copy(w2_hbm.at[layer, cols_of(blk), :], m2.at[blk], load_sem.at[blk, 1]))

    def input_copy(step):
        return pltpu.make_async_copy(x_hbm.at[step], hs.at[0], data_sem.at[0])

    def target_copy(step):
        return pltpu.make_async_copy(tgt_hbm.at[step], tgt, data_sem.at[1])

    wires = ((None, l1, r1_hbm, st1), (None, l2, r2_hbm, st2))

    def sends(step, blk, mat, src=None):
        out = []
        for slot, peer in enumerate(peers):
            out.append(pltpu.make_async_remote_copy(
                src_ref=wires[mat][1].at[blk] if src is None else src, dst_ref=wires[mat][2].at[step, slot, blk],
                send_sem=send_sem.at[blk, mat, slot], recv_sem=recv_sem.at[step, blk, mat, slot],
                device_id=peer, device_id_type=MESH))
        return out

    def start_sends(step, blk, mat, src=None):
        for cp in sends(step, blk, mat, src):
            cp.start()

    def sent_early(blk):
        layer, chunk = lax.div(blk, CHUNKS), lax.rem(blk, CHUNKS)
        return jnp.logical_and(chunk < CHUNKS - 1, layer > 0)

    def is_tail(blk):
        return jnp.logical_and(lax.rem(blk, CHUNKS) == CHUNKS - 1, blk >= CHUNKS)

    def tail_src(blk, mat):
        return (tail_one, tail_two)[mat].at[lax.max(lax.div(blk, CHUNKS) - 1, 0)]

    def wait_sent(step, blk, mats=(0, 1)):
        for mat in mats:
            for cp in sends(step, blk, mat):
                cp.wait_send()

    def tile_rows(i):
        return pl.ds(pl.multiple_of(i * TILE, TILE), TILE)

    def mix(step, blk, mats=(0, 1)):
        for mat in mats:
            for cp in sends(step, blk, mat):
                cp.wait_recv()
        stage = [pltpu.make_async_copy(wires[mat][2].at[step, slot, blk], wires[mat][3].at[slot], stage_sem.at[mat, slot])
                 for mat in mats for slot in range(3)]
        for cp in stage:
            cp.start()

        @pl.when(jnp.logical_not(is_tail(blk)))
        def _():
            wait_sent(step, blk, mats)

        for cp in stage:
            cp.wait()
        for mat in mats:
            _, lo, _, st = wires[mat]
            own, at = (m1, (lax.div(blk, CHUNKS), slice(None), cols_of(blk))) if mat == 0 else (m2, (blk,))
            other = st[2].astype(F32)
            new = (own[at] + st[0].astype(F32) + st[1].astype(F32) + other + other) * 0.2
            own[at] = new
            lo[blk] = new.astype(BF16)

    barrier = pltpu.get_barrier_semaphore()
    for peer in peers:
        pl.semaphore_signal(barrier, inc=1, device_id=peer, device_id_type=MESH)
    input_copy(0).start()

    for blk in range(CHUNKS):
        for cp in load_copies(blk):
            cp.start()
    target_copy(0).start()

    def first_forward():
        @pl.loop(0, n_layers)
        def _(layer):
            base = layer * CHUNKS

            @pl.when(layer < n_layers - 1)
            def _():
                for c in range(CHUNKS):
                    for cp in load_copies(lax.min(base + CHUNKS + c, n_blk - 1)):
                        cp.start()

            for c in range(CHUNKS):
                for cp in load_copies(base + c):
                    cp.wait()
                l1[base + c] = m1[layer, :, c * f_blk:(c + 1) * f_blk].astype(BF16)
                l2[base + c] = m2[base + c].astype(BF16)

            behind = None
            for rows in pieces + [None]:
                pre = []
                if rows is not None:
                    hid_f = hs[layer, rows, :].astype(F32)
                    n_lo = (hid_f * inv_rms_of(hid_f)).astype(BF16)
                    nrm[rows, :] = n_lo
                    pre = [matmul(n_lo, l1[base + c]) for c in range(CHUNKS)]
                if behind is not None:
                    b_rows, b_hid, b_act = behind
                    mlp = matmul(b_act[0], l2[base])
                    for c in range(1, CHUNKS):
                        mlp += matmul(b_act[c], l2[base + c])
                    hs[layer + 1, b_rows, :] = (b_hid + mlp).astype(BF16)
                if rows is not None:
                    b_act = [(z * gelu_half(z)[2]).astype(BF16) for z in pre]
                    act[rows, :] = b_act[0]
                    behind = (rows, hid_f, b_act)


    @pl.loop(0, n_steps)
    def _(step):
        input_copy(step).wait()

        @pl.when(step == 0)
        def _():
            first_forward()

        @pl.when(step > 0)
        def _():
            @pl.loop(0, n_blk)
            def _(k):
                blk = n_blk - CHUNKS - CHUNKS * lax.div(k, CHUNKS) + lax.rem(k, CHUNKS)

                @pl.when(sent_early(blk))
                def _():
                    mix(step - 1, blk)

        @pl.loop(0, lax.select(step > 0, n_blk, 0))
        def _(blk):
            layer, chunk = lax.div(blk, CHUNKS), lax.rem(blk, CHUNKS)
            last_blk = blk == n_blk - 1

            @pl.when(chunk == 0)
            def _():
                @pl.loop(0, n_tiles)
                def _(i):
                    rows = tile_rows(i)
                    hid_f = hs[layer, rows, :].astype(F32)
                    n_f = hid_f * inv_rms_of(hid_f)
                    nrm[rows, :] = n_f.astype(BF16)
                    acc[rows, :] = hid_f

            @pl.when(jnp.logical_not(jnp.logical_or(sent_early(blk), last_blk)))
            def _():
                mix(step - 1, blk)

            @pl.when(jnp.logical_not(last_blk))
            def _():
                keep = lax.select(blk == n_blk - CHUNKS, 0, 1)
                behind = None
                for rows in pieces + [None]:
                    if rows is not None:
                        pre = matmul(nrm[rows, :], l1[blk])
                    if behind is not None:
                        acc[behind[0], :] += matmul(behind[1], l2[blk])
                    if rows is not None:
                        a_lo = (pre * gelu_half(pre)[2]).astype(BF16)
                        ff[keep, rows, :] = a_lo
                        behind = (rows, a_lo)

            @pl.when(last_blk)
            def _():
                mix(step - 1, blk, (0,))
                for rows in pieces:
                    pre = matmul(nrm[rows, :], l1[blk])
                    dpre[rows, :] = (pre * gelu_half(pre)[2]).astype(BF16)
                mix(step - 1, blk, (1,))
                for rows in pieces:
                    hs[n_layers, rows, :] = (acc[rows, :] + matmul(dpre[rows, :], l2[blk])).astype(BF16)

            @pl.when(jnp.logical_and(chunk == CHUNKS - 1, layer < n_layers - 1))
            def _():
                @pl.loop(0, n_tiles)
                def _(i):
                    rows = tile_rows(i)
                    hs[layer + 1, rows, :] = acc[rows, :].astype(BF16)

        target_copy(step).wait()

        @pl.loop(0, n_tiles)
        def _(i):
            rows = tile_rows(i)
            hid = hs[n_layers, rows, :].astype(F32)
            e_f = (2.0 / (batch * d_model)) * (hid - tgt[rows, :].astype(F32))
            err[rows, :] = e_f
            err_lo[rows, :] = e_f.astype(BF16)
            err_t[:, rows] = e_f.T.astype(BF16)
            acc[rows, :] = jnp.zeros((TILE, d_model), F32)

        head_blk = n_blk - CHUNKS
        upd_head = m2[head_blk] - LEARN_RATE * matmul(err_t[...], act[...]).T
        m2[head_blk] = upd_head
        head_two[...] = upd_head.astype(BF16)

        @pl.when(step == 0)
        def _():
            pl.semaphore_wait(barrier, 3)

        at_once = jnp.logical_or(step > 0, lax.rem(row + col, 2) == 0)

        @pl.when(at_once)
        def _():
            start_sends(step, head_blk, 1, head_two)

        @pl.loop(0, n_tiles)
        def _(i):
            rows = tile_rows(i)
            nrm_t[:, rows] = nrm[rows, :].astype(F32).T.astype(BF16)

        @pl.loop(0, n_blk)
        def _(k):
            layer, chunk = n_layers - 1 - lax.div(k, CHUNKS), lax.rem(k, CHUNKS)
            blk = layer * CHUNKS + chunk

            @pl.when(jnp.logical_and(chunk == 0, k > 0))
            def _():
                @pl.loop(0, n_tiles)
                def _(i):
                    rows = tile_rows(i)
                    hid_f = hs[layer, rows, :].astype(F32)
                    n_f = hid_f * inv_rms_of(hid_f)
                    nrm[rows, :] = n_f.astype(BF16)
                    nrm_t[:, rows] = n_f.T.astype(BF16)
                    e_f = err[rows, :]
                    err_lo[rows, :] = e_f.astype(BF16)
                    err_t[:, rows] = e_f.T.astype(BF16)
                    acc[rows, :] = jnp.zeros((TILE, d_model), F32)

            @pl.loop(0, n_tiles)
            def _(i):
                rows = tile_rows(i)
                pre = matmul(nrm[rows, :], l1[blk])
                sq, t, half = gelu_half(pre)
                act[rows, :] = (pre * half).astype(BF16)
                slope = half + ((half * (1.0 - t)) * pre) * (GELU_C + (3.0 * GELU_C * GELU_K) * sq)
                d_pre = (matmul_t(err_lo[rows, :], l2[blk]) * slope).astype(BF16)
                dpre[rows, :] = d_pre
                acc[rows, :] += matmul_t(d_pre, l1[blk])

            @pl.when(k > 0)
            def _():
                upd_two = m2[blk] - LEARN_RATE * matmul(err_t[...], act[...]).T
                m2[blk] = upd_two
                l2[blk] = upd_two.astype(BF16)

                @pl.when(jnp.logical_and(k == 1, jnp.logical_not(at_once)))
                def _():
                    start_sends(step, head_blk, 1, head_two)
                    start_sends(step, head_blk, 0)

                @pl.when(sent_early(blk))
                def _():
                    start_sends(step, blk, 1)

            grad_one = matmul(nrm_t[...], dpre[...])
            upd_one = m1[layer, :, cols_of(blk)] - LEARN_RATE * grad_one
            m1[layer, :, cols_of(blk)] = upd_one
            l1[blk] = upd_one.astype(BF16)

            @pl.when(jnp.logical_and(sent_early(blk), jnp.logical_or(k > 0, at_once)))
            def _():
                start_sends(step, blk, 0)

            @pl.when(is_tail(blk))
            def _():
                @pl.when(step > 0)
                def _():
                    wait_sent(step - 1, blk)

                tail_src(blk, 0)[...] = l1[blk]
                tail_src(blk, 1)[...] = l2[blk]

            @pl.when(jnp.logical_and(chunk == CHUNKS - 1, layer > 0))
            def _():
                @pl.loop(0, n_tiles)
                def _(i):
                    rows = tile_rows(i)
                    hid_f = hs[layer, rows, :].astype(F32)
                    inv = inv_rms_of(hid_f)
                    n_f = hid_f * inv
                    d_n = acc[rows, :]
                    err[rows, :] += inv * (d_n - n_f * jnp.mean(d_n * n_f, axis=-1, keepdims=True))

        @pl.loop(0, n_blk)
        def _(blk):
            @pl.when(is_tail(blk))
            def _():
                for mat in range(2):
                    start_sends(step, blk, mat, tail_src(blk, mat))

            @pl.when(jnp.logical_not(jnp.logical_or(sent_early(blk), is_tail(blk))))
            def _():
                for mat in range(2):
                    start_sends(step, blk, mat)

        @pl.when(step < n_steps - 1)
        def _():
            input_copy(lax.min(step + 1, n_steps - 1)).start()
            target_copy(lax.min(step + 1, n_steps - 1)).start()

    for early in (True, False):
        @pl.loop(0, n_blk)
        def _(blk):
            turn = sent_early(blk) if early else jnp.logical_not(sent_early(blk))

            @pl.when(turn)
            def _():
                for mat in range(2):
                    mix(n_steps - 1, blk, (mat,))

    @pl.loop(0, n_blk)
    def _(blk):
        @pl.when(is_tail(blk))
        def _():
            wait_sent(n_steps - 1, blk)


def solution(mesh):
    n_rows = mesh.shape['row']
    n_cols = mesh.shape['col']

    def device_fn(w_one, w_two, inputs, targets):
        n_layers, d_model, d_ff = w_one.shape[2:]
        n_steps, batch = inputs.shape[2:4]
        f_blk = d_ff // CHUNKS
        n_blk = n_layers * CHUNKS
        dims = (n_rows, n_cols, n_steps, n_layers, batch, d_model, d_ff)
        any_spec = pl.BlockSpec(memory_space=pl.ANY)
        vmem_spec = pl.BlockSpec(memory_space=pltpu.VMEM)
        out = pl.pallas_call(
            functools.partial(kernel, dims),
            out_shape=(
                pltpu.VMEM((n_layers, d_model, d_ff), F32),
                pltpu.VMEM((n_blk, f_blk, d_model), F32),
                jax.ShapeDtypeStruct((n_steps, 3, n_blk, d_model, f_blk), BF16),
                jax.ShapeDtypeStruct((n_steps, 3, n_blk, f_blk, d_model), BF16),
            ),
            in_specs=[any_spec] * 4,
            out_specs=(vmem_spec, vmem_spec, any_spec, any_spec),
            scratch_shapes=[
                pltpu.VMEM((n_blk, d_model, f_blk), BF16),
                pltpu.VMEM((n_blk, f_blk, d_model), BF16),
                pltpu.VMEM((n_layers + 1, batch, d_model), BF16),
                pltpu.VMEM((batch, d_model), F32),
                pltpu.VMEM((batch, d_model), F32),
                pltpu.VMEM((batch, d_model), BF16),
                pltpu.VMEM((2, batch, f_blk), BF16),
                pltpu.VMEM((batch, d_model), BF16),
                pltpu.VMEM((batch, d_model), BF16),
                pltpu.VMEM((d_model, batch), BF16),
                pltpu.VMEM((d_model, batch), BF16),
                pltpu.VMEM((f_blk, d_model), BF16),
                pltpu.VMEM((n_layers - 1, d_model, f_blk), BF16),
                pltpu.VMEM((n_layers - 1, f_blk, d_model), BF16),
                pltpu.VMEM((3, d_model, f_blk), BF16),
                pltpu.VMEM((3, f_blk, d_model), BF16),
                pltpu.SemaphoreType.DMA((n_blk, 2)),
                pltpu.SemaphoreType.DMA((2,)),
                pltpu.SemaphoreType.DMA((2, 3)),
                pltpu.SemaphoreType.DMA((n_blk, 2, 3)),
                pltpu.SemaphoreType.DMA((n_steps, n_blk, 2, 3)),
            ],
            compiler_params=pltpu.CompilerParams(
                collective_id=0, has_side_effects=True, vmem_limit_bytes=VMEM_BYTES),
            name="gossip_sgd",
        )(w_one[0, 0], w_two[0, 0], inputs[0, 0], targets[0, 0])
        return out[0][None, None], out[1].reshape(w_two.shape)

    grid_spec = P('row', 'col')
    return jax.shard_map(device_fn, mesh=mesh, in_specs=(grid_spec,) * 4, out_specs=(grid_spec, grid_spec), check_vma=False)
```

```python
import functools

import jax
import jax.numpy as jnp
from jax import lax
from jax.experimental import pallas as pl
from jax.experimental.pallas import tpu as pltpu
from jax.sharding import PartitionSpec as P

LEARN_RATE = 1.5
NORM_EPS = 1e-6
GELU_C = 0.7978845608028654
GELU_K = 0.044715

MESH = pl.DeviceIdType.MESH
F32 = jnp.float32
BF16 = jnp.bfloat16
CHUNKS = 3
TILE = 512
VMEM_BYTES = 47_000_000
SUB = 256


def matmul(lhs, rhs):
    return jnp.dot(lhs, rhs, preferred_element_type=F32)


def matmul_t(lhs, rhs):
    return lax.dot_general(lhs, rhs, (((1,), (1,)), ((), ())), preferred_element_type=F32)


def gelu_half(pre_act):
    sq = pre_act * pre_act
    t = jnp.tanh(pre_act * (GELU_C + (GELU_C * GELU_K) * sq))
    return sq, t, 0.5 + 0.5 * t


def inv_rms_of(hid_f):
    return lax.rsqrt(jnp.mean(hid_f * hid_f, axis=-1, keepdims=True) + NORM_EPS)


def kernel(dims, w1_hbm, w2_hbm, x_hbm, tgt_hbm, m1, m2, r1_hbm, r2_hbm,
           l1, l2, hs, err, acc, tgt, ff, nrm, err_lo, nrm_t, err_t, head_two, tail_one, tail_two, st1, st2,
           load_sem, data_sem, stage_sem, send_sem, recv_sem):
    n_rows, n_cols, n_steps, n_layers, batch, d_model, d_ff = dims
    f_blk = d_ff // CHUNKS
    n_blk = n_layers * CHUNKS
    n_tiles = batch // TILE
    act, dpre = ff.at[0], ff.at[1]
    pieces = [slice(i, i + SUB) for i in range(0, batch, SUB)]
    row, col = lax.axis_index("row"), lax.axis_index("col")
    peers = ((row, lax.rem(col + 1, n_cols)), (row, lax.rem(col + n_cols - 1, n_cols)), (n_rows - 1 - row, col))

    def cols_of(blk):
        return pl.ds(pl.multiple_of(lax.rem(blk, CHUNKS) * f_blk, f_blk), f_blk)

    def load_copies(blk):
        layer = lax.div(blk, CHUNKS)
        return (pltpu.make_async_copy(w1_hbm.at[layer, :, cols_of(blk)], m1.at[layer, :, cols_of(blk)], load_sem.at[blk, 0]),
                pltpu.make_async_copy(w2_hbm.at[layer, cols_of(blk), :], m2.at[blk], load_sem.at[blk, 1]))

    def input_copy(step):
        return pltpu.make_async_copy(x_hbm.at[step], hs.at[0], data_sem.at[0])

    def target_copy(step):
        return pltpu.make_async_copy(tgt_hbm.at[step], tgt, data_sem.at[1])

    wires = ((None, l1, r1_hbm, st1), (None, l2, r2_hbm, st2))

    def sends(step, blk, mat, src=None):
        out = []
        for slot, peer in enumerate(peers):
            out.append(pltpu.make_async_remote_copy(
                src_ref=wires[mat][1].at[blk] if src is None else src, dst_ref=wires[mat][2].at[step, slot, blk],
                send_sem=send_sem.at[blk, mat, slot], recv_sem=recv_sem.at[step, blk, mat, slot],
                device_id=peer, device_id_type=MESH))
        return out

    def start_sends(step, blk, mat, src=None):
        for cp in sends(step, blk, mat, src):
            cp.start()

    def sent_early(blk):
        layer, chunk = lax.div(blk, CHUNKS), lax.rem(blk, CHUNKS)
        return jnp.logical_and(chunk < CHUNKS - 1, layer > 0)

    def is_tail(blk):
        return jnp.logical_and(lax.rem(blk, CHUNKS) == CHUNKS - 1, blk >= CHUNKS)

    def tail_src(blk, mat):
        return (tail_one, tail_two)[mat].at[lax.max(lax.div(blk, CHUNKS) - 1, 0)]

    def wait_sent(step, blk, mats=(0, 1)):
        for mat in mats:
            for cp in sends(step, blk, mat):
                cp.wait_send()

    def tile_rows(i):
        return pl.ds(pl.multiple_of(i * TILE, TILE), TILE)

    def mix(step, blk, mats=(0, 1)):
        for mat in mats:
            for cp in sends(step, blk, mat):
                cp.wait_recv()
        stage = [pltpu.make_async_copy(wires[mat][2].at[step, slot, blk], wires[mat][3].at[slot], stage_sem.at[mat, slot])
                 for mat in mats for slot in range(3)]
        for cp in stage:
            cp.start()

        @pl.when(jnp.logical_not(is_tail(blk)))
        def _():
            wait_sent(step, blk, mats)

        for cp in stage:
            cp.wait()
        for mat in mats:
            _, lo, _, st = wires[mat]
            own, at = (m1, (lax.div(blk, CHUNKS), slice(None), cols_of(blk))) if mat == 0 else (m2, (blk,))
            other = st[2].astype(F32)
            new = (own[at] + st[0].astype(F32) + st[1].astype(F32) + other + other) * 0.2
            own[at] = new
            lo[blk] = new.astype(BF16)

    barrier = pltpu.get_barrier_semaphore()
    for peer in peers:
        pl.semaphore_signal(barrier, inc=1, device_id=peer, device_id_type=MESH)
    input_copy(0).start()

    for blk in range(CHUNKS):
        for cp in load_copies(blk):
            cp.start()
    target_copy(0).start()

    def loss_grad(rows, hid, size):
        e_f = (2.0 / (batch * d_model)) * (hid.astype(F32) - tgt[rows, :].astype(F32))
        err[rows, :] = e_f
        err_lo[rows, :] = e_f.astype(BF16)
        err_t[:, rows] = e_f.T.astype(BF16)
        acc[rows, :] = jnp.zeros((size, d_model), F32)

    def first_forward():
        @pl.loop(0, n_layers)
        def _(layer):
            base = layer * CHUNKS

            @pl.when(layer < n_layers - 1)
            def _():
                for c in range(CHUNKS):
                    for cp in load_copies(lax.min(base + CHUNKS + c, n_blk - 1)):
                        cp.start()

            for c in range(CHUNKS):
                for cp in load_copies(base + c):
                    cp.wait()
                l1[base + c] = m1[layer, :, c * f_blk:(c + 1) * f_blk].astype(BF16)
                l2[base + c] = m2[base + c].astype(BF16)

            behind = None
            for rows in pieces + [None]:
                pre = []
                if rows is not None:
                    hid_f = hs[layer, rows, :].astype(F32)
                    n_lo = (hid_f * inv_rms_of(hid_f)).astype(BF16)
                    nrm[rows, :] = n_lo
                    pre = [matmul(n_lo, l1[base + c]) for c in range(CHUNKS)]
                if behind is not None:
                    b_rows, b_hid, b_act = behind
                    mlp = matmul(b_act[0], l2[base])
                    for c in range(1, CHUNKS):
                        mlp += matmul(b_act[c], l2[base + c])
                    hs[layer + 1, b_rows, :] = (b_hid + mlp).astype(BF16)
                if rows is not None:
                    b_act = [(z * gelu_half(z)[2]).astype(BF16) for z in pre]
                    act[rows, :] = b_act[0]
                    behind = (rows, hid_f, b_act)


    @pl.loop(0, n_steps)
    def _(step):
        input_copy(step).wait()

        @pl.when(step == 0)
        def _():
            first_forward()

        @pl.when(step > 0)
        def _():
            @pl.loop(0, n_blk)
            def _(k):
                blk = n_blk - CHUNKS - CHUNKS * lax.div(k, CHUNKS) + lax.rem(k, CHUNKS)

                @pl.when(sent_early(blk))
                def _():
                    mix(step - 1, blk)

        @pl.loop(0, lax.select(step > 0, n_blk, 0))
        def _(blk):
            layer, chunk = lax.div(blk, CHUNKS), lax.rem(blk, CHUNKS)
            last_blk = blk == n_blk - 1

            @pl.when(chunk == 0)
            def _():
                @pl.loop(0, n_tiles)
                def _(i):
                    rows = tile_rows(i)
                    hid_f = hs[layer, rows, :].astype(F32)
                    n_f = hid_f * inv_rms_of(hid_f)
                    nrm[rows, :] = n_f.astype(BF16)
                    acc[rows, :] = hid_f

            @pl.when(jnp.logical_not(jnp.logical_or(sent_early(blk), last_blk)))
            def _():
                mix(step - 1, blk)

            @pl.when(jnp.logical_not(last_blk))
            def _():
                keep = lax.select(blk == n_blk - CHUNKS, 0, 1)
                behind = None
                for rows in pieces + [None]:
                    if rows is not None:
                        pre = matmul(nrm[rows, :], l1[blk])
                    if behind is not None:
                        acc[behind[0], :] += matmul(behind[1], l2[blk])
                    if rows is not None:
                        a_lo = (pre * gelu_half(pre)[2]).astype(BF16)
                        ff[keep, rows, :] = a_lo
                        behind = (rows, a_lo)

            @pl.when(last_blk)
            def _():
                mix(step - 1, blk, (0,))
                for rows in pieces:
                    pre = matmul(nrm[rows, :], l1[blk])
                    dpre[rows, :] = (pre * gelu_half(pre)[2]).astype(BF16)
                target_copy(step).wait()
                mix(step - 1, blk, (1,))
                for rows in pieces:
                    loss_grad(rows, (acc[rows, :] + matmul(dpre[rows, :], l2[blk])).astype(BF16), SUB)

            @pl.when(jnp.logical_and(chunk == CHUNKS - 1, layer < n_layers - 1))
            def _():
                @pl.loop(0, n_tiles)
                def _(i):
                    rows = tile_rows(i)
                    hs[layer + 1, rows, :] = acc[rows, :].astype(BF16)

        @pl.when(step == 0)
        def _():
            target_copy(0).wait()

            @pl.loop(0, n_tiles)
            def _(i):
                rows = tile_rows(i)
                loss_grad(rows, hs[n_layers, rows, :], TILE)

        head_blk = n_blk - CHUNKS
        upd_head = m2[head_blk] - LEARN_RATE * matmul(err_t[...], act[...]).T
        m2[head_blk] = upd_head
        head_two[...] = upd_head.astype(BF16)

        @pl.when(step == 0)
        def _():
            pl.semaphore_wait(barrier, 3)

        at_once = jnp.logical_or(step > 0, lax.rem(row + col, 2) == 0)

        @pl.when(at_once)
        def _():
            start_sends(step, head_blk, 1, head_two)

        @pl.loop(0, n_tiles)
        def _(i):
            rows = tile_rows(i)
            nrm_t[:, rows] = nrm[rows, :].astype(F32).T.astype(BF16)

        @pl.loop(0, n_blk)
        def _(k):
            layer, chunk = n_layers - 1 - lax.div(k, CHUNKS), lax.rem(k, CHUNKS)
            blk = layer * CHUNKS + chunk

            @pl.when(jnp.logical_and(chunk == 0, k > 0))
            def _():
                @pl.loop(0, n_tiles)
                def _(i):
                    rows = tile_rows(i)
                    hid_f = hs[layer, rows, :].astype(F32)
                    n_f = hid_f * inv_rms_of(hid_f)
                    nrm[rows, :] = n_f.astype(BF16)
                    nrm_t[:, rows] = n_f.T.astype(BF16)
                    e_f = err[rows, :]
                    err_lo[rows, :] = e_f.astype(BF16)
                    err_t[:, rows] = e_f.T.astype(BF16)
                    acc[rows, :] = jnp.zeros((TILE, d_model), F32)

            behind = None
            for rows in pieces + [None]:
                if rows is not None:
                    pre = matmul(nrm[rows, :], l1[blk])
                    d_act = matmul_t(err_lo[rows, :], l2[blk])
                if behind is not None:
                    acc[behind[0], :] += matmul_t(behind[1], l1[blk])
                if rows is not None:
                    sq, t, half = gelu_half(pre)
                    act[rows, :] = (pre * half).astype(BF16)
                    slope = half + ((half * (1.0 - t)) * pre) * (GELU_C + (3.0 * GELU_C * GELU_K) * sq)
                    d_pre = (d_act * slope).astype(BF16)
                    dpre[rows, :] = d_pre
                    behind = (rows, d_pre)

            @pl.when(k > 0)
            def _():
                upd_two = m2[blk] - LEARN_RATE * matmul(err_t[...], act[...]).T
                m2[blk] = upd_two
                l2[blk] = upd_two.astype(BF16)

                @pl.when(jnp.logical_and(k == 1, jnp.logical_not(at_once)))
                def _():
                    start_sends(step, head_blk, 1, head_two)
                    start_sends(step, head_blk, 0)

                @pl.when(sent_early(blk))
                def _():
                    start_sends(step, blk, 1)

            grad_one = matmul(nrm_t[...], dpre[...])
            upd_one = m1[layer, :, cols_of(blk)] - LEARN_RATE * grad_one
            m1[layer, :, cols_of(blk)] = upd_one
            l1[blk] = upd_one.astype(BF16)

            @pl.when(jnp.logical_and(sent_early(blk), jnp.logical_or(k > 0, at_once)))
            def _():
                start_sends(step, blk, 0)

            @pl.when(is_tail(blk))
            def _():
                @pl.when(step > 0)
                def _():
                    wait_sent(step - 1, blk)

                tail_src(blk, 0)[...] = l1[blk]
                tail_src(blk, 1)[...] = l2[blk]

            @pl.when(jnp.logical_and(chunk == CHUNKS - 1, layer > 0))
            def _():
                @pl.loop(0, n_tiles)
                def _(i):
                    rows = tile_rows(i)
                    hid_f = hs[layer, rows, :].astype(F32)
                    inv = inv_rms_of(hid_f)
                    n_f = hid_f * inv
                    d_n = acc[rows, :]
                    err[rows, :] += inv * (d_n - n_f * jnp.mean(d_n * n_f, axis=-1, keepdims=True))

        @pl.loop(0, n_blk)
        def _(blk):
            @pl.when(is_tail(blk))
            def _():
                for mat in range(2):
                    start_sends(step, blk, mat, tail_src(blk, mat))

            @pl.when(jnp.logical_not(jnp.logical_or(sent_early(blk), is_tail(blk))))
            def _():
                for mat in range(2):
                    start_sends(step, blk, mat)

        @pl.when(step < n_steps - 1)
        def _():
            input_copy(lax.min(step + 1, n_steps - 1)).start()
            target_copy(lax.min(step + 1, n_steps - 1)).start()

    for early in (True, False):
        @pl.loop(0, n_blk)
        def _(blk):
            turn = sent_early(blk) if early else jnp.logical_not(sent_early(blk))

            @pl.when(turn)
            def _():
                for mat in range(2):
                    mix(n_steps - 1, blk, (mat,))

    @pl.loop(0, n_blk)
    def _(blk):
        @pl.when(is_tail(blk))
        def _():
            wait_sent(n_steps - 1, blk)


def solution(mesh):
    n_rows = mesh.shape['row']
    n_cols = mesh.shape['col']

    def device_fn(w_one, w_two, inputs, targets):
        n_layers, d_model, d_ff = w_one.shape[2:]
        n_steps, batch = inputs.shape[2:4]
        f_blk = d_ff // CHUNKS
        n_blk = n_layers * CHUNKS
        dims = (n_rows, n_cols, n_steps, n_layers, batch, d_model, d_ff)
        any_spec = pl.BlockSpec(memory_space=pl.ANY)
        vmem_spec = pl.BlockSpec(memory_space=pltpu.VMEM)
        out = pl.pallas_call(
            functools.partial(kernel, dims),
            out_shape=(
                pltpu.VMEM((n_layers, d_model, d_ff), F32),
                pltpu.VMEM((n_blk, f_blk, d_model), F32),
                jax.ShapeDtypeStruct((n_steps, 3, n_blk, d_model, f_blk), BF16),
                jax.ShapeDtypeStruct((n_steps, 3, n_blk, f_blk, d_model), BF16),
            ),
            in_specs=[any_spec] * 4,
            out_specs=(vmem_spec, vmem_spec, any_spec, any_spec),
            scratch_shapes=[
                pltpu.VMEM((n_blk, d_model, f_blk), BF16),
                pltpu.VMEM((n_blk, f_blk, d_model), BF16),
                pltpu.VMEM((n_layers + 1, batch, d_model), BF16),
                pltpu.VMEM((batch, d_model), F32),
                pltpu.VMEM((batch, d_model), F32),
                pltpu.VMEM((batch, d_model), BF16),
                pltpu.VMEM((2, batch, f_blk), BF16),
                pltpu.VMEM((batch, d_model), BF16),
                pltpu.VMEM((batch, d_model), BF16),
                pltpu.VMEM((d_model, batch), BF16),
                pltpu.VMEM((d_model, batch), BF16),
                pltpu.VMEM((f_blk, d_model), BF16),
                pltpu.VMEM((n_layers - 1, d_model, f_blk), BF16),
                pltpu.VMEM((n_layers - 1, f_blk, d_model), BF16),
                pltpu.VMEM((3, d_model, f_blk), BF16),
                pltpu.VMEM((3, f_blk, d_model), BF16),
                pltpu.SemaphoreType.DMA((n_blk, 2)),
                pltpu.SemaphoreType.DMA((2,)),
                pltpu.SemaphoreType.DMA((2, 3)),
                pltpu.SemaphoreType.DMA((n_blk, 2, 3)),
                pltpu.SemaphoreType.DMA((n_steps, n_blk, 2, 3)),
            ],
            compiler_params=pltpu.CompilerParams(
                collective_id=0, has_side_effects=True, vmem_limit_bytes=VMEM_BYTES),
            name="gossip_sgd",
        )(w_one[0, 0], w_two[0, 0], inputs[0, 0], targets[0, 0])
        return out[0][None, None], out[1].reshape(w_two.shape)

    grid_spec = P('row', 'col')
    return jax.shard_map(device_fn, mesh=mesh, in_specs=(grid_spec,) * 4, out_specs=(grid_spec, grid_spec), check_vma=False)
```

```python
import functools

import jax
import jax.numpy as jnp
from jax import lax
from jax.experimental import pallas as pl
from jax.experimental.pallas import tpu as pltpu
from jax.sharding import PartitionSpec as P

LEARN_RATE = 1.5
NORM_EPS = 1e-6
GELU_C = 0.7978845608028654
GELU_K = 0.044715

MESH = pl.DeviceIdType.MESH
F32 = jnp.float32
BF16 = jnp.bfloat16
CHUNKS = 3
TILE = 512
VMEM_BYTES = 47_000_000
SUB = 256


def matmul(lhs, rhs):
    return jnp.dot(lhs, rhs, preferred_element_type=F32)


def matmul_t(lhs, rhs):
    return lax.dot_general(lhs, rhs, (((1,), (1,)), ((), ())), preferred_element_type=F32)


def gelu_half(pre_act):
    sq = pre_act * pre_act
    t = jnp.tanh(pre_act * (GELU_C + (GELU_C * GELU_K) * sq))
    return sq, t, 0.5 + 0.5 * t


def inv_rms_of(hid_f):
    return lax.rsqrt(jnp.mean(hid_f * hid_f, axis=-1, keepdims=True) + NORM_EPS)


def kernel(dims, w1_hbm, w2_hbm, x_hbm, tgt_hbm, m1, m2, r1_hbm, r2_hbm,
           l1, l2, hs, err, acc, tgt, ff, nrm, err_lo, nrm_t, err_t, head_two, tail_one, tail_two, last_two, st1, st2,
           load_sem, data_sem, stage_sem, send_sem, recv_sem):
    n_rows, n_cols, n_steps, n_layers, batch, d_model, d_ff = dims
    f_blk = d_ff // CHUNKS
    n_blk = n_layers * CHUNKS
    n_tiles = batch // TILE
    act, dpre = ff.at[0], ff.at[1]
    pieces = [slice(i, i + SUB) for i in range(0, batch, SUB)]
    row, col = lax.axis_index("row"), lax.axis_index("col")
    peers = ((row, lax.rem(col + 1, n_cols)), (row, lax.rem(col + n_cols - 1, n_cols)), (n_rows - 1 - row, col))

    def cols_of(blk):
        return pl.ds(pl.multiple_of(lax.rem(blk, CHUNKS) * f_blk, f_blk), f_blk)

    def load_copies(blk):
        layer = lax.div(blk, CHUNKS)
        return (pltpu.make_async_copy(w1_hbm.at[layer, :, cols_of(blk)], m1.at[layer, :, cols_of(blk)], load_sem.at[blk, 0]),
                pltpu.make_async_copy(w2_hbm.at[layer, cols_of(blk), :], m2.at[blk], load_sem.at[blk, 1]))

    def input_copy(step):
        return pltpu.make_async_copy(x_hbm.at[step], hs.at[0], data_sem.at[0])

    def target_copy(step):
        return pltpu.make_async_copy(tgt_hbm.at[step], tgt, data_sem.at[1])

    wires = ((None, l1, r1_hbm, st1), (None, l2, r2_hbm, st2))

    def sends(step, blk, mat, src=None, dst=None):
        out = []
        for slot, peer in enumerate(peers):
            out.append(pltpu.make_async_remote_copy(
                src_ref=wires[mat][1].at[blk] if src is None else src, dst_ref=wires[mat][2].at[step, slot, blk] if dst is None else dst.at[slot],
                send_sem=send_sem.at[blk, mat, slot], recv_sem=recv_sem.at[step, blk, mat, slot],
                device_id=peer, device_id_type=MESH))
        return out

    def start_sends(step, blk, mat, src=None, dst=None):
        for cp in sends(step, blk, mat, src, dst):
            cp.start()

    def sent_early(blk):
        layer, chunk = lax.div(blk, CHUNKS), lax.rem(blk, CHUNKS)
        return jnp.logical_and(chunk < CHUNKS - 1, layer > 0)

    def is_tail(blk):
        return jnp.logical_and(lax.rem(blk, CHUNKS) == CHUNKS - 1, blk >= CHUNKS)

    def tail_src(blk, mat):
        return (tail_one, tail_two)[mat].at[lax.max(lax.div(blk, CHUNKS) - 1, 0)]

    def wait_sent(step, blk, mats=(0, 1)):
        for mat in mats:
            for cp in sends(step, blk, mat):
                cp.wait_send()

    def tile_rows(i):
        return pl.ds(pl.multiple_of(i * TILE, TILE), TILE)

    def mix(step, blk, mats=(0, 1)):
        for mat in mats:
            for cp in sends(step, blk, mat):
                cp.wait_recv()
        stage = [pltpu.make_async_copy(wires[mat][2].at[step, slot, blk], wires[mat][3].at[slot], stage_sem.at[mat, slot])
                 for mat in mats for slot in range(3)]
        for cp in stage:
            cp.start()

        @pl.when(jnp.logical_not(is_tail(blk)))
        def _():
            wait_sent(step, blk, mats)

        for cp in stage:
            cp.wait()
        for mat in mats:
            _, lo, _, st = wires[mat]
            own, at = (m1, (lax.div(blk, CHUNKS), slice(None), cols_of(blk))) if mat == 0 else (m2, (blk,))
            other = st[2].astype(F32)
            new = (own[at] + st[0].astype(F32) + st[1].astype(F32) + other + other) * 0.2
            own[at] = new
            lo[blk] = new.astype(BF16)

    barrier = pltpu.get_barrier_semaphore()
    for peer in peers:
        pl.semaphore_signal(barrier, inc=1, device_id=peer, device_id_type=MESH)
    input_copy(0).start()

    for blk in range(CHUNKS):
        for cp in load_copies(blk):
            cp.start()
    target_copy(0).start()

    def loss_grad(rows, hid, size):
        e_f = (2.0 / (batch * d_model)) * (hid.astype(F32) - tgt[rows, :].astype(F32))
        err[rows, :] = e_f
        err_lo[rows, :] = e_f.astype(BF16)
        err_t[:, rows] = e_f.T.astype(BF16)
        acc[rows, :] = jnp.zeros((size, d_model), F32)

    def first_forward():
        @pl.loop(0, n_layers)
        def _(layer):
            base = layer * CHUNKS

            @pl.when(layer < n_layers - 1)
            def _():
                for c in range(CHUNKS):
                    for cp in load_copies(lax.min(base + CHUNKS + c, n_blk - 1)):
                        cp.start()

            for c in range(CHUNKS):
                for cp in load_copies(base + c):
                    cp.wait()
                l1[base + c] = m1[layer, :, c * f_blk:(c + 1) * f_blk].astype(BF16)
                l2[base + c] = m2[base + c].astype(BF16)

            behind = None
            for rows in pieces + [None]:
                pre = []
                if rows is not None:
                    hid_f = hs[layer, rows, :].astype(F32)
                    n_lo = (hid_f * inv_rms_of(hid_f)).astype(BF16)
                    nrm[rows, :] = n_lo
                    pre = [matmul(n_lo, l1[base + c]) for c in range(CHUNKS)]
                if behind is not None:
                    b_rows, b_hid, b_act = behind
                    mlp = matmul(b_act[0], l2[base])
                    for c in range(1, CHUNKS):
                        mlp += matmul(b_act[c], l2[base + c])
                    hs[layer + 1, b_rows, :] = (b_hid + mlp).astype(BF16)
                if rows is not None:
                    b_act = [(z * gelu_half(z)[2]).astype(BF16) for z in pre]
                    act[rows, :] = b_act[0]
                    behind = (rows, hid_f, b_act)


    @pl.loop(0, n_steps)
    def _(step):
        input_copy(step).wait()

        @pl.when(step == 0)
        def _():
            first_forward()

        @pl.when(step > 0)
        def _():
            @pl.loop(0, n_blk)
            def _(k):
                blk = n_blk - CHUNKS - CHUNKS * lax.div(k, CHUNKS) + lax.rem(k, CHUNKS)

                @pl.when(sent_early(blk))
                def _():
                    mix(step - 1, blk)

        @pl.loop(0, lax.select(step > 0, n_blk, 0))
        def _(blk):
            layer, chunk = lax.div(blk, CHUNKS), lax.rem(blk, CHUNKS)
            last_blk = blk == n_blk - 1

            @pl.when(chunk == 0)
            def _():
                @pl.loop(0, n_tiles)
                def _(i):
                    rows = tile_rows(i)
                    hid_f = hs[layer, rows, :].astype(F32)
                    n_f = hid_f * inv_rms_of(hid_f)
                    nrm[rows, :] = n_f.astype(BF16)
                    acc[rows, :] = hid_f

            @pl.when(jnp.logical_not(jnp.logical_or(sent_early(blk), last_blk)))
            def _():
                mix(step - 1, blk)

            @pl.when(jnp.logical_not(last_blk))
            def _():
                keep = lax.select(blk == n_blk - CHUNKS, 0, 1)
                behind = None
                for rows in pieces + [None]:
                    if rows is not None:
                        pre = matmul(nrm[rows, :], l1[blk])
                    if behind is not None:
                        acc[behind[0], :] += matmul(behind[1], l2[blk])
                    if rows is not None:
                        a_lo = (pre * gelu_half(pre)[2]).astype(BF16)
                        ff[keep, rows, :] = a_lo
                        behind = (rows, a_lo)

            @pl.when(last_blk)
            def _():
                mix(step - 1, blk, (0,))
                for rows in pieces:
                    pre = matmul(nrm[rows, :], l1[blk])
                    dpre[rows, :] = (pre * gelu_half(pre)[2]).astype(BF16)
                target_copy(step).wait()
                mix(step - 1, blk, (1,))
                for rows in pieces:
                    loss_grad(rows, (acc[rows, :] + matmul(dpre[rows, :], l2[blk])).astype(BF16), SUB)

            @pl.when(jnp.logical_and(chunk == CHUNKS - 1, layer < n_layers - 1))
            def _():
                @pl.loop(0, n_tiles)
                def _(i):
                    rows = tile_rows(i)
                    hs[layer + 1, rows, :] = acc[rows, :].astype(BF16)

        @pl.when(step == 0)
        def _():
            target_copy(0).wait()

            @pl.loop(0, n_tiles)
            def _(i):
                rows = tile_rows(i)
                loss_grad(rows, hs[n_layers, rows, :], TILE)

        head_blk = n_blk - CHUNKS
        upd_head = m2[head_blk] - LEARN_RATE * matmul(err_t[...], act[...]).T
        m2[head_blk] = upd_head
        head_two[...] = upd_head.astype(BF16)

        @pl.when(step == 0)
        def _():
            pl.semaphore_wait(barrier, 3)

        at_once = jnp.logical_or(step > 0, lax.rem(row + col, 2) == 0)

        @pl.when(at_once)
        def _():
            start_sends(step, head_blk, 1, head_two)

        @pl.loop(0, n_tiles)
        def _(i):
            rows = tile_rows(i)
            nrm_t[:, rows] = nrm[rows, :].astype(F32).T.astype(BF16)

        @pl.loop(0, n_blk)
        def _(k):
            layer, chunk = n_layers - 1 - lax.div(k, CHUNKS), lax.rem(k, CHUNKS)
            blk = layer * CHUNKS + chunk

            @pl.when(jnp.logical_and(chunk == 0, k > 0))
            def _():
                @pl.loop(0, n_tiles)
                def _(i):
                    rows = tile_rows(i)
                    hid_f = hs[layer, rows, :].astype(F32)
                    n_f = hid_f * inv_rms_of(hid_f)
                    nrm[rows, :] = n_f.astype(BF16)
                    nrm_t[:, rows] = n_f.T.astype(BF16)
                    e_f = err[rows, :]
                    err_lo[rows, :] = e_f.astype(BF16)
                    err_t[:, rows] = e_f.T.astype(BF16)
                    acc[rows, :] = jnp.zeros((TILE, d_model), F32)

            behind = None
            for rows in pieces + [None]:
                if rows is not None:
                    pre = matmul(nrm[rows, :], l1[blk])
                    d_act = matmul_t(err_lo[rows, :], l2[blk])
                if behind is not None:
                    acc[behind[0], :] += matmul_t(behind[1], l1[blk])
                if rows is not None:
                    sq, t, half = gelu_half(pre)
                    act[rows, :] = (pre * half).astype(BF16)
                    slope = half + ((half * (1.0 - t)) * pre) * (GELU_C + (3.0 * GELU_C * GELU_K) * sq)
                    d_pre = (d_act * slope).astype(BF16)
                    dpre[rows, :] = d_pre
                    behind = (rows, d_pre)

            @pl.when(k > 0)
            def _():
                upd_two = m2[blk] - LEARN_RATE * matmul(err_t[...], act[...]).T
                m2[blk] = upd_two
                l2[blk] = upd_two.astype(BF16)

                @pl.when(jnp.logical_and(k == 1, jnp.logical_not(at_once)))
                def _():
                    start_sends(step, head_blk, 1, head_two)
                    start_sends(step, head_blk, 0)

                @pl.when(sent_early(blk))
                def _():
                    start_sends(step, blk, 1)

            grad_one = matmul(nrm_t[...], dpre[...])
            upd_one = m1[layer, :, cols_of(blk)] - LEARN_RATE * grad_one
            m1[layer, :, cols_of(blk)] = upd_one
            l1[blk] = upd_one.astype(BF16)

            @pl.when(jnp.logical_and(sent_early(blk), jnp.logical_or(k > 0, at_once)))
            def _():
                start_sends(step, blk, 0)

            @pl.when(is_tail(blk))
            def _():
                @pl.when(step > 0)
                def _():
                    wait_sent(step - 1, blk)

                tail_src(blk, 0)[...] = l1[blk]
                tail_src(blk, 1)[...] = l2[blk]

            @pl.when(jnp.logical_and(chunk == CHUNKS - 1, layer > 0))
            def _():
                @pl.loop(0, n_tiles)
                def _(i):
                    rows = tile_rows(i)
                    hid_f = hs[layer, rows, :].astype(F32)
                    inv = inv_rms_of(hid_f)
                    n_f = hid_f * inv
                    d_n = acc[rows, :]
                    err[rows, :] += inv * (d_n - n_f * jnp.mean(d_n * n_f, axis=-1, keepdims=True))

        @pl.loop(0, n_blk)
        def _(blk):
            @pl.when(is_tail(blk))
            def _():
                final = jnp.logical_and(step == n_steps - 1, blk == n_blk - 1)
                start_sends(step, blk, 0, tail_src(blk, 0))

                @pl.when(jnp.logical_not(final))
                def _():
                    start_sends(step, blk, 1, tail_src(blk, 1))

                @pl.when(final)
                def _():
                    start_sends(step, blk, 1, tail_src(blk, 1), last_two)

            @pl.when(jnp.logical_not(jnp.logical_or(sent_early(blk), is_tail(blk))))
            def _():
                for mat in range(2):
                    start_sends(step, blk, mat)

        @pl.when(step < n_steps - 1)
        def _():
            input_copy(lax.min(step + 1, n_steps - 1)).start()
            target_copy(lax.min(step + 1, n_steps - 1)).start()

    for early in (True, False):
        @pl.loop(0, n_blk)
        def _(blk):
            turn = sent_early(blk) if early else jnp.logical_not(sent_early(blk))

            @pl.when(turn)
            def _():
                mix(n_steps - 1, blk, (0,))

                @pl.when(blk < n_blk - 1)
                def _():
                    mix(n_steps - 1, blk, (1,))

    for cp in sends(n_steps - 1, n_blk - 1, 1, None, last_two):
        cp.wait_recv()
    other = last_two[2].astype(F32)
    m2[n_blk - 1] = (m2[n_blk - 1] + last_two[0].astype(F32) + last_two[1].astype(F32) + other + other) * 0.2

    @pl.loop(0, n_blk)
    def _(blk):
        @pl.when(is_tail(blk))
        def _():
            wait_sent(n_steps - 1, blk)


def solution(mesh):
    n_rows = mesh.shape['row']
    n_cols = mesh.shape['col']

    def device_fn(w_one, w_two, inputs, targets):
        n_layers, d_model, d_ff = w_one.shape[2:]
        n_steps, batch = inputs.shape[2:4]
        f_blk = d_ff // CHUNKS
        n_blk = n_layers * CHUNKS
        dims = (n_rows, n_cols, n_steps, n_layers, batch, d_model, d_ff)
        any_spec = pl.BlockSpec(memory_space=pl.ANY)
        vmem_spec = pl.BlockSpec(memory_space=pltpu.VMEM)
        out = pl.pallas_call(
            functools.partial(kernel, dims),
            out_shape=(
                pltpu.VMEM((n_layers, d_model, d_ff), F32),
                pltpu.VMEM((n_blk, f_blk, d_model), F32),
                jax.ShapeDtypeStruct((n_steps, 3, n_blk, d_model, f_blk), BF16),
                jax.ShapeDtypeStruct((n_steps, 3, n_blk, f_blk, d_model), BF16),
            ),
            in_specs=[any_spec] * 4,
            out_specs=(vmem_spec, vmem_spec, any_spec, any_spec),
            scratch_shapes=[
                pltpu.VMEM((n_blk, d_model, f_blk), BF16),
                pltpu.VMEM((n_blk, f_blk, d_model), BF16),
                pltpu.VMEM((n_layers + 1, batch, d_model), BF16),
                pltpu.VMEM((batch, d_model), F32),
                pltpu.VMEM((batch, d_model), F32),
                pltpu.VMEM((batch, d_model), BF16),
                pltpu.VMEM((2, batch, f_blk), BF16),
                pltpu.VMEM((batch, d_model), BF16),
                pltpu.VMEM((batch, d_model), BF16),
                pltpu.VMEM((d_model, batch), BF16),
                pltpu.VMEM((d_model, batch), BF16),
                pltpu.VMEM((f_blk, d_model), BF16),
                pltpu.VMEM((n_layers - 1, d_model, f_blk), BF16),
                pltpu.VMEM((n_layers - 1, f_blk, d_model), BF16),
                pltpu.VMEM((3, f_blk, d_model), BF16),
                pltpu.VMEM((3, d_model, f_blk), BF16),
                pltpu.VMEM((3, f_blk, d_model), BF16),
                pltpu.SemaphoreType.DMA((n_blk, 2)),
                pltpu.SemaphoreType.DMA((2,)),
                pltpu.SemaphoreType.DMA((2, 3)),
                pltpu.SemaphoreType.DMA((n_blk, 2, 3)),
                pltpu.SemaphoreType.DMA((n_steps, n_blk, 2, 3)),
            ],
            compiler_params=pltpu.CompilerParams(
                collective_id=0, has_side_effects=True, vmem_limit_bytes=VMEM_BYTES),
            name="gossip_sgd",
        )(w_one[0, 0], w_two[0, 0], inputs[0, 0], targets[0, 0])
        return out[0][None, None], out[1].reshape(w_two.shape)

    grid_spec = P('row', 'col')
    return jax.shard_map(device_fn, mesh=mesh, in_specs=(grid_spec,) * 4, out_specs=(grid_spec, grid_spec), check_vma=False)
```
